32 devices in a mesh: ep: 8 (over z, y), dp: 4 (over x, core).
Axes of the slice: x: 2, y: 2, z: 4, core: 2. Of those that a mesh axis runs over, the one named last changes fastest.
Arguments:
- tokens: bfloat16 [6144, 2880], P(('ep', 'dp')), may hold values from -64 to 64
- out_grad: bfloat16 [6144, 2880], P(('ep', 'dp')), may hold values from -6 to 6
- indices: int32 [6144, 4], P(('ep', 'dp')), may hold values from 0 to 31, as said below
- expert_rows: bfloat16 [4, 32, 8, 36, 2880], P('dp', 'ep'), may hold values from -0.111328125 to 0.111328125
- router_weight: bfloat16 [2880, 32], replicated, may hold values from -1 to 1
- router_bias: float32 [32], replicated, may hold values from -3 to 3
- balance_scale: float32 [1], replicated, may hold values from 64 to 256
Outputs:
- token_grad: bfloat16 [6144, 2880], P(('ep', 'dp'))
- weight_grad: float32 [2880, 32], P('dp', 'ep')
- balance_loss: float32 [1], replicated
The draws below stay inside these ranges and needn't reach their ends.
Inputs may be any that keep to these rules, and one draw needn't show every extreme that they name: `indices`: each row names 4 different experts. Within the 192 rows of one device no expert is named by more than 36 rows, and some expert is named by exactly 36 rows. Within the rows of one device the 4 experts of one ep index (experts j * 4 to j * 4 + 3) are named by at most 108 rows together, and those of some ep index by exactly 108. Every expert is named by some row of every device.
All inputs are finite; a program needn't handle non-finite values.
Results may differ from the reference program's by a relative error of at most 0.0014.
The reference program's roundings to bfloat16 on the way (of `picked` and `logit_grad`) count: a program that leaves them out, or rounds other values in their place, can miss the bound.
Values may be sent and summed in bfloat16 or wider, within the bound.
No kernel may reach another device: no remote copies, remote signals or barrier semaphores. Data moves between devices by JAX's collectives and lax.ppermute only.
A program may use at most 128 MiB of HBM per device.

```python
import math
import jax
import jax.numpy as jnp
from jax import lax

D = 2880
K = 4
EXP_DEV = 4
TOK_DEV = 192
E = 32
CAP = 36
TOKENS = 6144
N_EP = 8
N_DP = 4


def router_table(key):
    sub_key = jax.random.fold_in(key, 11)
    scale = D ** (-0.5)
    return jnp.clip(jax.random.normal(sub_key, (D, E), jnp.float32) * scale, -6.0 * scale, 6.0 * scale)


def draw_router_weight(key, part):
    return router_table(key).astype(jnp.bfloat16)


def block_offsets(key, table_rows):
    pick_key = jax.random.fold_in(key, 29)
    picks = jax.random.randint(pick_key, (N_EP * N_DP, 8), 0, E)
    columns = jnp.take(table_rows.T, picks.reshape(-1), axis=0).reshape(N_EP * N_DP, 8, D)
    per_block = 4.0 * jnp.sum(columns, axis=1)
    return jnp.repeat(per_block, TOK_DEV, axis=0)


def draw_tokens(key, part):
    sub_key = jax.random.fold_in(key, 23)
    table_rows = router_table(key)
    shifted = block_offsets(key, table_rows)
    result = jnp.clip(jax.random.normal(sub_key, (TOKENS, D), jnp.float32), -6.0, 6.0) + shifted
    return jnp.clip(result, -64.0, 64.0).astype(jnp.bfloat16)


def route_block(block_key, common_key):
    key_shift, key_rows, key_cols = jax.random.split(block_key, 3)
    key_heavy, key_inner = jax.random.split(common_key, 2)
    third = CAP // 3
    group_order = jax.random.permutation(key_heavy, N_EP)
    heavy = (group_order % 2 == 0)[:, None]
    shift = jax.random.randint(key_shift, (N_EP, 1), 0, third + 1)
    heavy_loads = jnp.concatenate([jnp.full((N_EP, 2), CAP, jnp.int32), 2 * third - shift, third + shift], axis=1)
    light_loads = jnp.concatenate([jnp.full((N_EP, 1), CAP, jnp.int32), 2 * third - shift, third + shift, jnp.full((N_EP, 1), third, jnp.int32)], axis=1)
    pattern = jnp.where(heavy, heavy_loads, light_loads).astype(jnp.int32)
    inner_scores = jax.random.randint(key_inner, (N_EP, EXP_DEV), 0, 1 << 20) * EXP_DEV + jnp.arange(EXP_DEV, dtype=jnp.int32)[None, :]
    inner_order = jnp.argsort(inner_scores, axis=1)
    loads = jnp.take_along_axis(pattern, inner_order, axis=1).reshape(E)
    bounds = jnp.cumsum(loads)
    positions = jnp.arange(TOK_DEV * K, dtype=jnp.int32)
    labels = jnp.searchsorted(bounds, positions, side='right').astype(jnp.int32)
    grid = labels.reshape(K, TOK_DEV).T
    row_order = jax.random.permutation(key_rows, TOK_DEV)
    grid = jnp.take(grid, row_order, axis=0)
    col_scores = jax.random.randint(key_cols, (TOK_DEV, K), 0, 1 << 20) * K + jnp.arange(K, dtype=jnp.int32)[None, :]
    col_order = jnp.argsort(col_scores, axis=1)
    return jnp.take_along_axis(grid, col_order, axis=1).astype(jnp.int32)


def draw_indices(key, part):
    base_key = jax.random.fold_in(key, 37)
    common_key = jax.random.fold_in(key, 41)
    block_ids = jnp.arange(N_EP * N_DP, dtype=jnp.int32)
    blocks = jax.vmap(lambda block_id: route_block(jax.random.fold_in(base_key, block_id), common_key))(block_ids)
    return blocks.reshape(TOKENS, K).astype(jnp.int32)


def block_levels(key, extent, shards, least, largest):
    factor_of, own = 1.0, jax.random.fold_in(key, 6)
    for position, parts in shards:
        draws = jnp.exp(jax.random.uniform(jax.random.fold_in(own, position), (parts,), jnp.float32, least / len(shards), largest / len(shards)))
        factor_of = factor_of * jnp.repeat(draws, extent[position] // parts).reshape([-1 if axis == position else 1 for axis in range(len(extent))])
    return factor_of


def gaussian(stream_key, extent, scale, bound, pieces=(), kind=jnp.bfloat16):
    entries = jax.random.normal(stream_key, extent, jnp.float32) * scale
    if len(pieces) > 0:
        entries = block_levels(stream_key, extent, pieces, -0.22, 0.18) * entries
    return jnp.clip(entries, min=-bound, max=bound).astype(kind)


def setup_inputs(seed: int = 0) -> dict:
    splits = jax.random.split(jax.random.key(seed), 8)
    return {
        "tokens": draw_tokens(jax.random.fold_in(splits[7], 71), 0),
        "out_grad": gaussian(splits[1], (TOKENS, D), 1.0, 6.0, ((0, 32),)),
        "indices": draw_indices(jax.random.fold_in(splits[7], 71), 0),
        "expert_rows": gaussian(splits[3], (N_DP, E, N_EP, CAP, D), (D ** -0.5), 0.111328125, ((0, 4), (1, 8))),
        "router_weight": draw_router_weight(jax.random.fold_in(splits[7], 71), 0),
        "router_bias": gaussian(splits[5], (E,), 0.5, 3.0, (), jnp.float32),
        "balance_scale": jnp.clip(jnp.exp(jax.random.uniform(splits[6], (1,), jnp.float32, math.log(64.0), math.log(256.0))), 64.0, 256.0),
    }


def reference(tokens, out_grad, indices, expert_rows, router_weight, router_bias, balance_scale):
    logits = jnp.dot(tokens, router_weight, preferred_element_type=jnp.float32) + router_bias
    probability = jax.nn.softmax(logits, axis=-1)
    expert_ids = jnp.arange(E, dtype=jnp.int32)
    onehot = (indices[:, :, None] == expert_ids[None, None, :]).astype(jnp.float32)
    counts = lax.optimization_barrier(jnp.sum(onehot, axis=(0, 1)))
    prob_mean = lax.optimization_barrier(jnp.sum(probability, axis=0)) / TOKENS
    share_of = counts / (TOKENS * K)
    balance_loss = (E * jnp.sum(share_of * prob_mean)).reshape(1)

    def block_dots(block_id):
        ep_index = block_id // N_DP
        dp_index = block_id % N_DP
        cotangent = lax.dynamic_slice_in_dim(out_grad, block_id * TOK_DEV, TOK_DEV, 0)
        chosen_ids = lax.dynamic_slice_in_dim(indices, block_id * TOK_DEV, TOK_DEV, 0)
        group_rows = lax.dynamic_index_in_dim(expert_rows, dp_index, 0, keepdims=False)
        table_rows = lax.dynamic_index_in_dim(group_rows, ep_index, 1, keepdims=False)
        named_by = lax.optimization_barrier(jnp.sum((chosen_ids[:, :, None] == expert_ids[None, None, :]).astype(jnp.int32), axis=1))
        before = jnp.cumsum(named_by, axis=0) - named_by
        slot_index = jnp.take_along_axis(before, chosen_ids, axis=1)
        row_index = (chosen_ids * CAP + slot_index).astype(jnp.int32)
        picked = table_rows.reshape(E * CAP, D)[row_index]
        return jnp.einsum('td,tkd->tk', cotangent.astype(jnp.float32), picked.astype(jnp.float32))
    pair_dots = lax.map(block_dots, jnp.arange(N_EP * N_DP, dtype=jnp.int32)).reshape(TOKENS, K)
    chosen_logits = jnp.take_along_axis(logits, indices, axis=1)
    mix_weight = jax.nn.softmax(chosen_logits, axis=-1)
    sel_grad = mix_weight * (pair_dots - lax.optimization_barrier(jnp.sum(mix_weight * pair_dots, axis=1, keepdims=True)))
    balance_push = balance_scale[0] * E * share_of
    spread = probability * (balance_push[None, :] - lax.optimization_barrier(jnp.sum(probability * balance_push[None, :], axis=1, keepdims=True)))
    logit_grad = (spread + lax.optimization_barrier(jnp.sum(onehot * sel_grad[:, :, None], axis=1))).astype(jnp.bfloat16)
    token_grad = jnp.dot(logit_grad, router_weight.T, preferred_element_type=jnp.float32).astype(jnp.bfloat16)
    weight_grad = jnp.dot(tokens.T, logit_grad, preferred_element_type=jnp.float32) / math.sqrt(TOKENS)
    return (token_grad, weight_grad, balance_loss)
```

```python
import math

import jax
import jax.numpy as jnp
from jax import lax
from jax.experimental import pallas as pl
from jax.experimental.pallas import tpu as pltpu
from jax.sharding import PartitionSpec as P

F32, BF16 = jnp.float32, jnp.bfloat16


def split_rows(table, sel, count):
    total, width = table.shape
    step, block_in = sel.shape[0] // count, sel.shape[1]
    steps = total // block_in

    def body(sel_ref, x_ref, *outs):
        y = jnp.dot(sel_ref[...], x_ref[...], preferred_element_type=F32).astype(BF16)
        for c in range(count):
            outs[c][...] = y[c * step:(c + 1) * step]

    return pl.pallas_call(
        body,
        grid=(steps,),
        in_specs=[pl.BlockSpec(sel.shape, lambda i: (0, 0)), pl.BlockSpec((block_in, width), lambda i: (i, 0))],
        out_specs=[pl.BlockSpec((step, width), lambda i: (i, 0))] * count,
        out_shape=[jax.ShapeDtypeStruct((step * steps, width), BF16)] * count,
        cost_estimate=pl.CostEstimate(flops=2 * sel.size * width * steps, bytes_accessed=3 * total * width, transcendentals=0),
        name="split_rows",
    )(sel, table)


def dots_of(where, blocks, rows, pick, exp_dev):
    tok, wide = blocks[0].shape
    count, width = rows.shape
    cap = count // exp_dev

    def body(where_ref, *refs):
        block_refs = refs[:len(blocks)]
        rows_ref, pick_ref, out_ref, held, sem = refs[len(blocks):]
        out_ref[...] = jnp.zeros_like(out_ref)
        for i, block in enumerate(block_refs):
            @pl.when(where_ref[0] == i)
            def _(block=block):
                copy = pltpu.make_async_copy(block, held, sem)
                copy.start()
                copy.wait()

        @pl.when((where_ref[0] >= 0) & (where_ref[0] < len(blocks)))
        def _():
            nt = (((1,), (1,)), ((), ()))
            marks = lax.dot_general(pick_ref[...], held[:, width:], nt, preferred_element_type=F32).astype(jnp.int32)
            full = lax.dot_general(rows_ref[...], held[:, :width], nt, preferred_element_type=F32)
            slots = lax.broadcasted_iota(jnp.int32, (cap, tok), 0)
            for e in range(exp_dev):
                part = jnp.where(slots == marks[e:e + 1], full[e * cap:(e + 1) * cap], 0.0)
                out_ref[e:e + 1, :] = jnp.sum(part, axis=0, keepdims=True)

    return pl.pallas_call(
        body,
        in_specs=[pl.BlockSpec(memory_space=pltpu.SMEM)]
        + [pl.BlockSpec(memory_space=pl.ANY)] * len(blocks)
        + [pl.BlockSpec(memory_space=pltpu.VMEM)] * 2,
        out_specs=pl.BlockSpec(memory_space=pltpu.VMEM),
        out_shape=jax.ShapeDtypeStruct((exp_dev, tok), F32),
        scratch_shapes=[pltpu.VMEM((tok, wide), BF16), pltpu.SemaphoreType.DMA],
        cost_estimate=pl.CostEstimate(flops=2 * tok * count * width, bytes_accessed=2 * (tok + count) * width, transcendentals=0),
        name="dots_of",
    )(where, *blocks, rows, pick)


def on_device(tokens, out_grad, indices, expert_rows, router_weight, router_bias, balance_scale):
    tok, width = tokens.shape
    chosen = indices.shape[1]
    experts = router_weight.shape[1]
    exp_dev, capacity = expert_rows.shape[1], expert_rows.shape[3]
    ep, dp = lax.axis_size("ep"), lax.axis_size("dp")
    token_total = tok * ep * dp
    me = lax.axis_index("ep")
    side, place = me % 2, me // 2
    length = ep // 2
    reach = length // 2
    far = length - 1 - reach

    expert_ids = jnp.arange(experts, dtype=jnp.int32)
    onehot = (indices[:, :, None] == expert_ids[None, None, :]).astype(F32)
    named_by = jnp.sum(onehot, axis=1)
    row_ids = jnp.arange(tok, dtype=jnp.int32)
    lower_mask = (row_ids[:, None] > row_ids[None, :]).astype(BF16)
    before = jnp.dot(lower_mask, named_by.astype(BF16), preferred_element_type=F32)
    marks = jnp.where(named_by > 0, before, -1.0).astype(BF16)
    block = jnp.concatenate([out_grad, marks], axis=1)

    entries = exp_dev * capacity
    table = expert_rows.transpose(0, 1, 3, 2, 4).reshape(entries * ep, width)
    step = 16 if entries % 16 == 0 else entries
    r = jnp.arange(length * step, dtype=jnp.int32)[:, None]
    c = jnp.arange(step * ep, dtype=jnp.int32)[None, :]
    sel = lambda s: (c == (r % step) * ep + 2 * (r // step) + s).astype(BF16)
    leaving = split_rows(table, sel(1 - side), length)
    own = split_rows(table, sel(side), length)
    cross = [(j, j ^ 1) for j in range(ep)]
    order = [0, length - 1] + list(range(1, length - 1))
    other = [None] * length
    for s in order:
        other[s] = lax.ppermute(leaving[s], "ep", cross)

    def shift(x, by):
        pairs = [(2 * z + s, 2 * (z + by) + s) for z in range(length) if 0 <= z + by < length for s in range(2)]
        return lax.ppermute(x, "ep", pairs)

    below, above = [block], [block]
    for _ in range(reach):
        below.append(shift(below[-1], 1))
        above.append(shift(above[-1], -1))
    blocks = below[:0:-1] + [block] + above[1:]

    def rows_at(parts, index, valid):
        if len(valid) == 1:
            return parts[valid[0]]
        return lax.dynamic_index_in_dim(jnp.stack(parts), jnp.clip(index, 0, length - 1), 0, keepdims=False)

    visits = []
    for i in range(1, far + 1):
        d = reach + i
        for sign in (-1, 1):
            valid = [z + sign * d for z in range(length) if 0 <= z + sign * d < length]
            for kind, parts in ((0, own), (1, other)):
                visits.append((sign, i, kind, shift(rows_at(parts, place + sign * d, valid), sign * i)))

    iota8 = jnp.arange(8, dtype=jnp.int32)[:, None]

    def picker(column, kind):
        j = 2 * column + jnp.where(kind == 0, side, 1 - side)
        return ((expert_ids[None, :] == j * exp_dev + iota8) & (iota8 < exp_dev)).astype(BF16)

    answers = []
    for s in range(length):
        where = (s - place + reach).astype(jnp.int32).reshape(1)
        main = [dots_of(where, blocks, rows[s], picker(place, kind), exp_dev) for kind, rows in ((0, own), (1, other))]
        answers.append(main + [jnp.zeros((2 * exp_dev * far, tok), F32)])
    answers = jnp.stack([jnp.concatenate(a, axis=0) for a in answers])
    guests = {-1: [None] * (2 * far), 1: [None] * (2 * far)}
    for sign, i, kind, rows in visits:
        which = 0 if sign < 0 else 2 * reach
        got = dots_of(jnp.zeros((1,), jnp.int32), [blocks[which]], rows, picker(place - sign * i, kind), exp_dev)
        guests[sign][2 * (i - 1) + kind] = got
    source = jnp.arange(length, dtype=jnp.int32)[:, None, None]
    if far:
        guest = jnp.where(source == place - reach, jnp.concatenate(guests[-1], axis=0)[None], 0.0)
        guest = guest + jnp.where(source == place + reach, jnp.concatenate(guests[1], axis=0)[None], 0.0)
        answers = answers.at[:, 2 * exp_dev:].set(guest)

    counts_dp = jnp.sum(lax.all_gather(jnp.sum(named_by, axis=0), "dp"), axis=0)
    lanes = jnp.broadcast_to(counts_dp[None, None, None, :], (length, 2, answers.shape[1], experts))
    sides = jnp.arange(2, dtype=jnp.int32)[None, :, None, None]
    message = jnp.where(sides == side, answers[:, None], 0.0)
    message = jnp.concatenate([message, lanes], axis=3).reshape(ep, answers.shape[1], tok + experts)
    got = lax.all_to_all(message, "ep", split_axis=0, concat_axis=0, tiled=True)
    counts = jnp.sum(got[:, 0, tok:], axis=0)
    got = jnp.sum(got[:, :, :tok].reshape(length, 2, answers.shape[1], tok), axis=1)
    columns = got[:, :2 * exp_dev]
    for i in range(1, far + 1):
        part = got[:, 2 * exp_dev * i:2 * exp_dev * (i + 1)]
        empty = jnp.zeros_like(part[:i])
        columns = columns + jnp.concatenate([empty, jnp.where(source > place, part, 0.0)[:length - i]], axis=0)
        columns = columns + jnp.concatenate([jnp.where(source < place, part, 0.0)[i:], empty], axis=0)
    columns = columns.reshape(length, 2, exp_dev, tok)
    dots = jnp.where(side == 0, columns, columns[:, ::-1]).reshape(experts, tok)

    logits = jnp.dot(tokens, router_weight, preferred_element_type=F32) + router_bias
    probability = jax.nn.softmax(logits, axis=-1)
    share_of = counts / (token_total * chosen)
    pair_dots = jnp.sum(onehot * dots.T[:, None, :], axis=2)
    chosen_logits = jnp.sum(onehot * logits[:, None, :], axis=2)
    mix_weight = jax.nn.softmax(chosen_logits, axis=-1)
    sel_grad = mix_weight * (pair_dots - jnp.sum(mix_weight * pair_dots, axis=1, keepdims=True))
    balance_push = balance_scale[0] * experts * share_of
    spread = probability * (
        balance_push[None, :] - jnp.sum(probability * balance_push[None, :], axis=1, keepdims=True)
    )
    logit_grad = (spread + jnp.sum(onehot * sel_grad[:, :, None], axis=1)).astype(BF16)
    token_grad = lax.dot_general(
        logit_grad, router_weight, (((1,), (1,)), ((), ())), preferred_element_type=F32
    ).astype(BF16)
    piece = width // dp
    lanes_out = -(-(piece + experts) // 128) * 128
    prob_sums = jnp.sum(probability, axis=0)
    terms = []
    for d in range(dp):
        term = lax.dot_general(
            logit_grad, tokens[:, d * piece:(d + 1) * piece], (((0,), (0,)), ((), ())), preferred_element_type=F32
        ).reshape(ep, exp_dev, piece)
        sums = jnp.broadcast_to(prob_sums[None, None, :], (ep, exp_dev, experts))
        pad = jnp.zeros((ep, exp_dev, lanes_out - piece - experts), F32)
        terms.append(jnp.concatenate([term, sums, pad], axis=2))
    sent = jnp.stack(terms, axis=1).reshape(ep * dp, exp_dev, lanes_out)
    summed = jnp.sum(lax.all_to_all(sent, ("ep", "dp"), split_axis=0, concat_axis=0, tiled=True), axis=0)
    weight_grad = summed[:, :piece].T / math.sqrt(token_total)
    balance_loss = (experts * jnp.sum(share_of * (summed[0, piece:piece + experts] / token_total))).reshape(1)
    return (token_grad, weight_grad, balance_loss)


def solution(mesh):
    placed = (
        P(("ep", "dp"), None),
        P(("ep", "dp"), None),
        P(("ep", "dp"), None),
        P("dp", "ep", None, None, None),
        P(),
        P(),
        P(),
    )
    return jax.shard_map(
        on_device,
        mesh=mesh,
        in_specs=placed,
        out_specs=(P(("ep", "dp"), None), P("dp", "ep"), P()),
        check_vma=False,
    )
```

```python
import math

import jax
import jax.numpy as jnp
from jax import lax
from jax.experimental import pallas as pl
from jax.experimental.pallas import tpu as pltpu
from jax.sharding import PartitionSpec as P

F32, BF16 = jnp.float32, jnp.bfloat16


def split_rows(table, sel, count):
    total, width = table.shape
    rows, block_in = sel.shape[0] // count, sel.shape[1]
    parts = total // block_in
    group = max(g for g in (1, 2, 3) if parts % g == 0)

    def body(sel_ref, x_ref, *outs):
        for k in range(group):
            x = x_ref[k * block_in:(k + 1) * block_in, :]
            y = jnp.dot(sel_ref[...], x, preferred_element_type=F32).astype(BF16)
            for c in range(count):
                outs[c][k * rows:(k + 1) * rows, :] = y[c * rows:(c + 1) * rows]

    return pl.pallas_call(
        body,
        grid=(parts // group,),
        in_specs=[
            pl.BlockSpec(sel.shape, lambda i: (0, 0)),
            pl.BlockSpec((group * block_in, width), lambda i: (i, 0)),
        ],
        out_specs=[pl.BlockSpec((group * rows, width), lambda i: (i, 0))] * count,
        out_shape=[jax.ShapeDtypeStruct((rows * parts, width), BF16)] * count,
        cost_estimate=pl.CostEstimate(
            flops=2 * sel.size * width * parts, bytes_accessed=3 * total * width, transcendentals=0
        ),
        name="split_rows",
    )(sel, table)


NT = (((1,), (1,)), ((), ()))


def slot_dots(rows, block, pick, exp_dev, put):
    count, width = rows.shape
    tok, cap = block.shape[0], count // exp_dev
    marks = lax.dot_general(pick[...], block[:, width:], NT, preferred_element_type=F32).astype(jnp.int32)
    full = lax.dot_general(rows[...], block[:, :width], NT, preferred_element_type=F32)
    slots = lax.broadcasted_iota(jnp.int32, (cap, tok), 0)
    for e in range(exp_dev):
        part = jnp.where(slots == marks[e:e + 1], full[e * cap:(e + 1) * cap], 0.0)
        put(e, jnp.sum(part, axis=0, keepdims=True))


def meet(which, target, blocks, jobs, picks, counts, ep, height, exp_dev):
    tok, wide = blocks[0].shape
    experts = counts.shape[1]
    flat = [r for rows, _ in jobs for r in rows]
    count, width = flat[0].shape
    most = max(len(rows) for rows, _ in jobs)

    def body(which_ref, target_ref, *refs):
        block_refs, refs = refs[:len(blocks)], refs[len(blocks):]
        row_refs, refs = refs[:len(flat)], refs[len(flat):]
        picks_ref, counts_ref, out_ref, held, rows_held, block_sem, row_sem = refs
        first = [sum(len(rows) for rows, _ in jobs[:n]) for n in range(len(jobs))]

        def usable(n):
            return (which_ref[n] >= 0) & (which_ref[n] < len(blocks))

        def start(n):
            slot = n % 2
            for i, block in enumerate(block_refs):
                @pl.when(which_ref[n] == i)
                def _(block=block):
                    pltpu.make_async_copy(block, held.at[slot], block_sem.at[slot]).start()

            @pl.when(usable(n))
            def _():
                for k in range(len(jobs[n][0])):
                    pltpu.make_async_copy(row_refs[first[n] + k], rows_held.at[slot, k], row_sem.at[slot, k]).start()

        start(0)
        out_ref[...] = jnp.zeros_like(out_ref)
        out_ref[:, 0:1, tok:] = jnp.broadcast_to(counts_ref[...][None], (ep, 1, experts))
        for n in range(len(jobs)):
            if n + 1 < len(jobs):
                start(n + 1)
            slot = n % 2

            @pl.when(usable(n))
            def _(n=n, slot=slot):
                pltpu.make_async_copy(block_refs[0], held.at[slot], block_sem.at[slot]).wait()
                for k, line in enumerate(jobs[n][1]):
                    pltpu.make_async_copy(row_refs[0], rows_held.at[slot, k], row_sem.at[slot, k]).wait()
                    at = (first[n] + k) * 8

                    def put(e, value, line=line):
                        out_ref[pl.ds(target_ref[n], 1), line + e:line + e + 1, :tok] = value[None]

                    slot_dots(rows_held.at[slot, k], held.at[slot], picks_ref.at[at:at + 8], exp_dev, put)

    anywhere = pl.BlockSpec(memory_space=pl.ANY)
    scalars = pl.BlockSpec(memory_space=pltpu.SMEM)
    local = pl.BlockSpec(memory_space=pltpu.VMEM)
    return pl.pallas_call(
        body,
        in_specs=[scalars] * 2 + [anywhere] * (len(blocks) + len(flat)) + [local] * 2,
        out_specs=local,
        out_shape=jax.ShapeDtypeStruct((ep, height, tok + experts), F32),
        scratch_shapes=[
            pltpu.VMEM((2, tok, wide), BF16),
            pltpu.VMEM((2, most, count, width), BF16),
            pltpu.SemaphoreType.DMA((2,)),
            pltpu.SemaphoreType.DMA((2, most)),
        ],
        cost_estimate=pl.CostEstimate(
            flops=2 * len(flat) * tok * count * width, bytes_accessed=4 * len(flat) * count * width, transcendentals=0
        ),
        name="meet",
    )(which, target, *blocks, *flat, picks, counts)


def last_dots(block, rows, pick, exp_dev):
    tok = block.shape[0]

    def body(block_ref, rows_ref, pick_ref, out_ref):
        def put(e, value):
            out_ref[e:e + 1, :] = value

        slot_dots(rows_ref, block_ref, pick_ref, exp_dev, put)

    local = pl.BlockSpec(memory_space=pltpu.VMEM)
    return pl.pallas_call(
        body,
        in_specs=[local] * 3,
        out_specs=local,
        out_shape=jax.ShapeDtypeStruct((exp_dev, tok), F32),
        cost_estimate=pl.CostEstimate(
            flops=2 * tok * rows.size, bytes_accessed=2 * (block.size + rows.size), transcendentals=0
        ),
        name="last_dots",
    )(block, rows, pick)


def on_device(tokens, out_grad, indices, expert_rows, router_weight, router_bias, balance_scale):
    tok, width = tokens.shape
    chosen = indices.shape[1]
    experts = router_weight.shape[1]
    exp_dev, capacity = expert_rows.shape[1], expert_rows.shape[3]
    ep, dp = lax.axis_size("ep"), lax.axis_size("dp")
    token_total = tok * ep * dp
    me = lax.axis_index("ep")
    side, place = me % 2, me // 2
    length = ep // 2
    reach = length // 2
    far = length - 1 - reach

    expert_ids = jnp.arange(experts, dtype=jnp.int32)
    onehot = (indices[:, :, None] == expert_ids[None, None, :]).astype(F32)
    named_by = jnp.sum(onehot, axis=1)
    row_ids = jnp.arange(tok, dtype=jnp.int32)
    lower_mask = (row_ids[:, None] > row_ids[None, :]).astype(BF16)
    before = jnp.dot(lower_mask, named_by.astype(BF16), preferred_element_type=F32)
    marks = jnp.where(named_by > 0, before, -1.0).astype(BF16)
    block = jnp.concatenate([out_grad, marks], axis=1)

    low = place < length - reach
    away = jnp.arange(length - 1, -1, -1, dtype=jnp.int32)
    sources = (place + jnp.where(low, away, length - away)) % length

    entries = exp_dev * capacity
    table = expert_rows.transpose(0, 1, 3, 2, 4).reshape(entries * ep, width)
    step = 16 if entries % 16 == 0 else entries
    r = jnp.arange(step, dtype=jnp.int32)[None, :, None]
    c = jnp.arange(step * ep, dtype=jnp.int32)[None, None, :]
    sel = lambda s: (c == r * ep + 2 * sources[:, None, None] + s).astype(BF16).reshape(length * step, step * ep)
    leaving = split_rows(table, sel(1 - side), length)
    cross = [(j, j ^ 1) for j in range(ep)]
    other = [lax.ppermute(rows, "ep", cross) for rows in leaving]
    own = split_rows(table, sel(side), length)

    def shift(x, *moves):
        pairs = [(z, to) for valid, by in moves for z in range(length) for to in [z + by] if valid(z) and 0 <= to < length]
        return lax.ppermute(x, "ep", [(2 * z + s, 2 * to + s) for z, to in pairs for s in range(2)])

    below, above = [block], [block]
    for _ in range(reach):
        below.append(shift(below[-1], (lambda z: True, 1)))
        above.append(shift(above[-1], (lambda z: True, -1)))
    blocks = below[:0:-1] + [block] + above[1:]

    guests = []
    for i in range(1, far + 1):
        d = reach + i
        moves = ((lambda z: z + d < length, i), (lambda z: z - d >= 0, -i))
        guests.append([shift(rows[length - 1 - d], *moves) for rows in (own, other)])

    iota8 = jnp.arange(8, dtype=jnp.int32)[:, None]

    def picker(column, kind):
        j = 2 * column + (side if kind == 0 else 1 - side)
        return ((expert_ids[None, :] == j * exp_dev + iota8) & (iota8 < exp_dev)).astype(BF16)

    counts_dp = jnp.sum(lax.all_gather(jnp.sum(named_by, axis=0), "dp"), axis=0)[None]

    jobs, which, target, picks = [], [], [], []
    for n in range(length):
        kinds = (0, 1) if n < length - 1 else (0,)
        jobs.append(([(own, other)[kind][n] for kind in kinds], [exp_dev * kind for kind in kinds]))
        which.append(sources[n] - place + reach)
        target.append(2 * sources[n] + side)
        picks.extend(picker(place, kind) for kind in kinds)
    for i in range(1, far + 1):
        jobs.append((guests[i - 1], [exp_dev * (2 * i + kind) for kind in (0, 1)]))
        column = place + jnp.where(low, -i, i)
        there = (column >= 0) & (column < length)
        source = place + jnp.where(low, reach, -reach)
        which.append(jnp.where(there & (source >= 0) & (source < length), jnp.where(low, 2 * reach, 0), -1))
        target.append(jnp.clip(2 * source + side, 0, ep - 1))
        picks.extend(picker(column, kind) for kind in (0, 1))
    height = exp_dev * 2 * (1 + far)
    message = meet(
        jnp.stack(which).astype(jnp.int32), jnp.stack(target).astype(jnp.int32), blocks, jobs,
        jnp.concatenate(picks, axis=0), counts_dp, ep, height, exp_dev,
    )
    got = lax.all_to_all(message, "ep", split_axis=0, concat_axis=0, tiled=True)
    late = last_dots(block, other[length - 1], picker(place, 1), exp_dev)

    counts = jnp.sum(got[:, 0, tok:], axis=0)
    got = jnp.sum(got[:, :, :tok].reshape(length, 2, height, tok), axis=1)
    columns = got[:, :2 * exp_dev]
    at = jnp.arange(length, dtype=jnp.int32)[:, None, None]
    for i in range(1, far + 1):
        part = got[:, 2 * exp_dev * i:2 * exp_dev * (i + 1)]
        empty = jnp.zeros_like(part[:i])
        columns = columns + jnp.concatenate([empty, jnp.where(at > place, part, 0.0)[:length - i]], axis=0)
        columns = columns + jnp.concatenate([jnp.where(at < place, part, 0.0)[i:], empty], axis=0)
    columns = columns.reshape(length, 2, exp_dev, tok)
    columns = columns + jnp.where(at[..., None] == place, jnp.stack([jnp.zeros_like(late), late])[None], 0.0)
    dots = jnp.where(side == 0, columns, columns[:, ::-1]).reshape(experts, tok)

    tokens, _ = lax.optimization_barrier((tokens, block))
    logits = jnp.dot(tokens, router_weight, preferred_element_type=F32) + router_bias
    probability = jax.nn.softmax(logits, axis=-1)
    share_of = counts / (token_total * chosen)
    pair_dots = jnp.sum(onehot * dots.T[:, None, :], axis=2)
    chosen_logits = jnp.sum(onehot * logits[:, None, :], axis=2)
    mix_weight = jax.nn.softmax(chosen_logits, axis=-1)
    sel_grad = mix_weight * (pair_dots - jnp.sum(mix_weight * pair_dots, axis=1, keepdims=True))
    balance_push = balance_scale[0] * experts * share_of
    spread = probability * (
        balance_push[None, :] - jnp.sum(probability * balance_push[None, :], axis=1, keepdims=True)
    )
    logit_grad = (spread + jnp.sum(onehot * sel_grad[:, :, None], axis=1)).astype(BF16)
    token_grad = lax.dot_general(
        logit_grad, router_weight, (((1,), (1,)), ((), ())), preferred_element_type=F32
    ).astype(BF16)
    piece = width // dp
    lanes_out = -(-(piece + experts) // 128) * 128
    prob_sums = jnp.sum(probability, axis=0)
    terms = []
    for d in range(dp):
        term = lax.dot_general(
            logit_grad, tokens[:, d * piece:(d + 1) * piece], (((0,), (0,)), ((), ())), preferred_element_type=F32
        ).reshape(ep, exp_dev, piece)
        sums = jnp.broadcast_to(prob_sums[None, None, :], (ep, exp_dev, experts))
        pad = jnp.zeros((ep, exp_dev, lanes_out - piece - experts), F32)
        terms.append(jnp.concatenate([term, sums, pad], axis=2))
    sent = jnp.stack(terms, axis=1).reshape(ep * dp, exp_dev, lanes_out)
    summed = jnp.sum(lax.all_to_all(sent, ("ep", "dp"), split_axis=0, concat_axis=0, tiled=True), axis=0)
    weight_grad = summed[:, :piece].T / math.sqrt(token_total)
    balance_loss = (experts * jnp.sum(share_of * (summed[0, piece:piece + experts] / token_total))).reshape(1)
    return (token_grad, weight_grad, balance_loss)


def solution(mesh):
    placed = (
        P(("ep", "dp"), None),
        P(("ep", "dp"), None),
        P(("ep", "dp"), None),
        P("dp", "ep", None, None, None),
        P(),
        P(),
        P(),
    )
    return jax.shard_map(
        on_device,
        mesh=mesh,
        in_specs=placed,
        out_specs=(P(("ep", "dp"), None), P("dp", "ep"), P()),
        check_vma=False,
    )
```

```python
import math

import jax
import jax.numpy as jnp
from jax import lax
from jax.experimental import pallas as pl
from jax.experimental.pallas import tpu as pltpu
from jax.sharding import PartitionSpec as P

F32, BF16 = jnp.float32, jnp.bfloat16


NT = (((1,), (1,)), ((), ()))
ANYWHERE = pl.BlockSpec(memory_space=pl.ANY)
SCALARS = pl.BlockSpec(memory_space=pltpu.SMEM)
LOCAL = pl.BlockSpec(memory_space=pltpu.VMEM)


def split_rows(table, sels):
    total, width = table.shape
    count = len(sels)
    rows, block_in = sels[0].shape
    parts = total // block_in
    group = max(g for g in (1, 2, 3) if parts % g == 0)

    def body(sel_ref, x_ref, *outs):
        for k in range(group):
            x = x_ref[k * block_in:(k + 1) * block_in, :]
            y = jnp.dot(sel_ref[...], x, preferred_element_type=F32).astype(BF16)
            for c in range(count):
                outs[c][k * rows:(k + 1) * rows, :] = y[c * rows:(c + 1) * rows]

    return pl.pallas_call(
        body,
        grid=(parts // group,),
        in_specs=[
            pl.BlockSpec((count * rows, block_in), lambda i: (0, 0)),
            pl.BlockSpec((group * block_in, width), lambda i: (i, 0)),
        ],
        out_specs=[pl.BlockSpec((group * rows, width), lambda i: (i, 0))] * count,
        out_shape=[jax.ShapeDtypeStruct((rows * parts, width), BF16)] * count,
        cost_estimate=pl.CostEstimate(
            flops=2 * count * rows * block_in * width * parts, bytes_accessed=3 * total * width, transcendentals=0
        ),
        name="split_rows",
    )(jnp.concatenate(sels, axis=0), table)


def slot_dots(rows, block, marks, exp_dev, put):
    kinds, count, width = rows.shape
    tok, cap = block.shape[0], count // exp_dev
    if count % 16 == 0:
        full = lax.dot_general(rows[...].reshape(kinds * count, width), block[...], NT, preferred_element_type=F32)
        full = [full[k * count:(k + 1) * count] for k in range(kinds)]
    else:
        full = [lax.dot_general(rows[k], block[...], NT, preferred_element_type=F32) for k in range(kinds)]
    slots = lax.broadcasted_iota(jnp.int32, (cap, tok), 0)
    for kind, mark in enumerate(marks):
        mark = mark.astype(jnp.int32)
        for e in range(exp_dev):
            part = jnp.where(slots == mark[e:e + 1], full[kind][e * cap:(e + 1) * cap], 0.0)
            put(kind, e, jnp.sum(part, axis=0, keepdims=True))


def meet(scalars, blocks, jobs, marks, message, exp_dev):
    tok, width = blocks[0].shape
    flat = [r for rows, _ in jobs for r in rows]
    count = flat[0].shape[0]
    most = max(len(rows) for rows, _ in jobs)
    first = [sum(len(rows) for rows, _ in jobs[:n]) for n in range(len(jobs))]

    def body(scalar_ref, *refs):
        block_refs, refs = refs[:len(blocks)], refs[len(blocks):]
        row_refs, refs = refs[:len(flat)], refs[len(flat):]
        mark_refs, refs = refs[:len(jobs)], refs[len(jobs):]
        in_ref, out_ref, held, rows_held, block_sem, row_sem = refs

        def usable(n):
            return (scalar_ref[2 * n] >= 0) & (scalar_ref[2 * n] < len(blocks))

        def rows_copy(n, k):
            return pltpu.make_async_copy(row_refs[first[n] + k], rows_held.at[n % 2, k], row_sem.at[n % 2, k])

        def start(n):
            for i, block in enumerate(block_refs):
                @pl.when(scalar_ref[2 * n] == i)
                def _(block=block):
                    pltpu.make_async_copy(block, held.at[n % 2], block_sem.at[n % 2]).start()

            @pl.when(usable(n))
            def _():
                for k in range(len(jobs[n][0])):
                    rows_copy(n, k).start()

        start(0)
        out_ref[...] = in_ref[...]
        for n in range(len(jobs)):
            if n + 1 < len(jobs):
                start(n + 1)

            @pl.when(usable(n))
            def _(n=n):
                pltpu.make_async_copy(block_refs[0], held.at[n % 2], block_sem.at[n % 2]).wait()
                kinds = len(jobs[n][0])
                for k in range(kinds):
                    rows_copy(n, k).wait()

                def put(kind, e, value):
                    line = jobs[n][1] + kind * exp_dev + e
                    out_ref[pl.ds(scalar_ref[2 * n + 1], 1), line:line + 1, :] = value[None]

                each = [mark_refs[n][k] for k in range(kinds)]
                slot_dots(rows_held.at[n % 2, pl.ds(0, kinds)], held.at[n % 2], each, exp_dev, put)

    return pl.pallas_call(
        body,
        in_specs=[SCALARS] + [ANYWHERE] * (len(blocks) + len(flat)) + [LOCAL] * (len(jobs) + 1),
        out_specs=LOCAL,
        out_shape=jax.ShapeDtypeStruct(message.shape, F32),
        input_output_aliases={1 + len(blocks) + len(flat) + len(jobs): 0},
        scratch_shapes=[
            pltpu.VMEM((2, tok, width), BF16),
            pltpu.VMEM((2, most, count, width), BF16),
            pltpu.SemaphoreType.DMA((2,)),
            pltpu.SemaphoreType.DMA((2, most)),
        ],
        cost_estimate=pl.CostEstimate(
            flops=2 * len(flat) * tok * count * width, bytes_accessed=4 * len(flat) * count * width, transcendentals=0
        ),
        name="meet",
    )(scalars, *blocks, *flat, *marks, message)


def last_dots(block, rows, mark, exp_dev):
    tok = block.shape[0]

    def body(block_ref, rows_ref, mark_ref, out_ref):
        def put(kind, e, value):
            out_ref[e:e + 1, :] = value

        slot_dots(rows_ref, block_ref, [mark_ref[...]], exp_dev, put)

    return pl.pallas_call(
        body,
        in_specs=[LOCAL] * 3,
        out_specs=LOCAL,
        out_shape=jax.ShapeDtypeStruct((exp_dev, tok), F32),
        cost_estimate=pl.CostEstimate(
            flops=2 * tok * rows.size, bytes_accessed=2 * (block.size + rows.size), transcendentals=0
        ),
        name="last_dots",
    )(block, rows[None], mark)


def finish(spot, got, late, mix, spread, prob_sums, tokens, dp, exp_dev):
    experts, tok = mix.shape
    length, width = got.shape[0], tokens.shape[1]
    ep, piece = 2 * length, width // dp
    far = got.shape[1] // (2 * exp_dev) - 1
    lanes = -(-(piece + experts) // 128) * 128

    def body(spot_ref, got_ref, late_ref, mix_ref, spread_ref, sums_ref, tokens_ref, grad_ref, sent_ref, dots_ref):
        side, place = spot_ref[0], spot_ref[1]
        for c in range(length):
            for kind in range(2):
                value = got_ref[c, kind * exp_dev:(kind + 1) * exp_dev, :]
                for i in range(1, far + 1):
                    line = (2 * i + kind) * exp_dev
                    if c - i >= 0:
                        value += jnp.where(c - i > place, got_ref[c - i, line:line + exp_dev, :], 0.0)
                    if c + i < length:
                        value += jnp.where(c + i < place, got_ref[c + i, line:line + exp_dev, :], 0.0)
                if kind:
                    value += jnp.where(c == place, late_ref[...], 0.0)
                at = 2 * c + jnp.where(side == kind, 0, 1)
                dots_ref[pl.ds(at, 1), :, :] = value[None]
        dots = jnp.concatenate([dots_ref[j] for j in range(ep)], axis=0)
        mixed = mix_ref[...] * dots
        grad = (spread_ref[...] + (mixed - mix_ref[...] * jnp.sum(mixed, axis=0, keepdims=True))).astype(BF16)
        grad_ref[...] = grad
        term = jnp.dot(grad, tokens_ref[...], preferred_element_type=F32)
        for d in range(dp):
            part = term[:, d * piece:(d + 1) * piece]
            for j in range(ep):
                sent_ref[j * dp + d, :, :piece] = part[j * exp_dev:(j + 1) * exp_dev]
        sums = jnp.broadcast_to(sums_ref[...][None], (ep * dp, exp_dev, experts))
        sent_ref[:, :, piece:piece + experts] = sums
        if lanes > piece + experts:
            sent_ref[:, :, piece + experts:] = jnp.zeros((ep * dp, exp_dev, lanes - piece - experts), F32)

    return pl.pallas_call(
        body,
        in_specs=[SCALARS] + [LOCAL] * 6,
        out_specs=[LOCAL] * 2,
        out_shape=[
            jax.ShapeDtypeStruct((experts, tok), BF16),
            jax.ShapeDtypeStruct((ep * dp, exp_dev, lanes), F32),
        ],
        scratch_shapes=[pltpu.VMEM((ep, exp_dev, tok), F32)],
        cost_estimate=pl.CostEstimate(
            flops=2 * experts * tok * width, bytes_accessed=2 * tok * width + 4 * experts * width, transcendentals=0
        ),
        name="finish",
    )(spot, got, late, mix, spread, prob_sums, tokens)


def on_device(tokens, out_grad, indices, expert_rows, router_weight, router_bias, balance_scale):
    tok, width = tokens.shape
    chosen = indices.shape[1]
    experts = router_weight.shape[1]
    exp_dev, capacity = expert_rows.shape[1], expert_rows.shape[3]
    ep, dp = lax.axis_size("ep"), lax.axis_size("dp")
    token_total = tok * ep * dp
    me = lax.axis_index("ep")
    side, place = me % 2, me // 2
    length = ep // 2
    reach = length // 2
    far = length - 1 - reach

    low = place < length - reach
    away = jnp.arange(length - 1, -1, -1, dtype=jnp.int32)
    sources = (place + jnp.where(low, away, length - away)) % length

    entries = exp_dev * capacity
    table = expert_rows.transpose(0, 1, 3, 2, 4).reshape(entries * ep, width)
    step = 16 if entries % 16 == 0 else entries
    r = jnp.arange(step, dtype=jnp.int32)[:, None]
    c = jnp.arange(step * ep, dtype=jnp.int32)[None, :]
    leave = [(c == r * ep + 2 * sources[n] + 1 - side).astype(BF16) for n in range(length)]
    stay = [(c == r * ep + 2 * sources[n] + side).astype(BF16) for n in range(length)]
    cross = [(j, j ^ 1) for j in range(ep)]
    leaving = split_rows(table, leave[:1])
    block, table = lax.optimization_barrier((out_grad, leaving[0], table))[::2]
    rest = split_rows(table, leave[1:] + stay)
    leaving, own = leaving + rest[:length - 1], rest[length - 1:]
    other = [lax.ppermute(rows, "ep", cross) for rows in leaving]

    def shift(x, *moves):
        pairs = [(z, to) for valid, by in moves for z in range(length) for to in [z + by] if valid(z) and 0 <= to < length]
        return lax.ppermute(x, "ep", [(2 * z + s, 2 * to + s) for z, to in pairs for s in range(2)])

    below, above = [block], [block]
    for hop in range(reach):
        below.append(shift(below[-1], (lambda z: z >= hop, 1)))
        above.append(shift(above[-1], (lambda z: z + hop < length, -1)))
    blocks = below[:0:-1] + [block] + above[1:]

    guests = []
    for i in range(1, far + 1):
        d = reach + i
        moves = ((lambda z: z + d < length, i), (lambda z: z - d >= 0, -i))
        guests.append([shift(rows[length - 1 - d], *moves) for rows in (own, other)])

    expert_ids = jnp.arange(experts, dtype=jnp.int32)
    named = jnp.any(indices.T[:, None, :] == expert_ids[None, :, None], axis=0)
    row_ids = jnp.arange(tok, dtype=jnp.int32)
    earlier = (row_ids[:, None] < row_ids[None, :]).astype(BF16)
    before = jnp.dot(named.astype(BF16), earlier, preferred_element_type=F32)
    marks = jnp.where(named, before, -1.0).astype(BF16)
    marks = lax.all_to_all(jnp.broadcast_to(marks[None], (ep, experts, tok)), "ep", split_axis=0, concat_axis=0, tiled=True)
    counts = jnp.sum((marks >= 0).astype(F32), axis=(0, 2))
    counts = jnp.sum(lax.all_gather(counts, "dp"), axis=0)
    marks = marks.reshape(length, 2, length, 2, exp_dev, tok)
    marks = lax.dynamic_index_in_dim(marks, side, 1, keepdims=False)
    marks = jnp.where(side == 0, marks, marks[:, :, ::-1]).astype(F32)

    def marks_at(source, column):
        source, column = jnp.clip(source, 0, length - 1), jnp.clip(column, 0, length - 1)
        return lax.dynamic_slice(marks, (source, column, 0, 0, 0), (1, 1, 2, exp_dev, tok))[0, 0]

    def job(n, kinds, hops):
        at = marks_at(sources[n], place)[kinds[0]:kinds[-1] + 1]
        rows = [(own, other)[kind][n] for kind in kinds]
        return (rows, exp_dev * kinds[0]), at, (sources[n] - place + hops, sources[n])

    def guest_job(i):
        column = place + jnp.where(low, -i, i)
        source = place + jnp.where(low, reach, -reach)
        there = (column >= 0) & (column < length) & (source >= 0) & (source < length)
        which = jnp.where(there, jnp.where(low, 1, 0), -1)
        return (guests[i - 1], 2 * i * exp_dev), marks_at(source, column), (which, jnp.clip(source, 0, length - 1))

    message = jnp.zeros((length, 2 * exp_dev * (1 + far), tok), F32)
    near = {0: (0, 1), length - 2: (0,), length - 1: (0,)}
    calls = [(blocks[reach - 1:reach + 2], [job(n, kinds, 1) for n, kinds in near.items()])]
    middle = [job(n, (0, 1), reach) for n in range(1, length - 2)]
    calls.append((blocks, middle + [job(length - 2, (1,), reach)]))
    if far:
        calls.append((blocks[::2 * reach], [guest_job(i) for i in range(1, far + 1)]))
    for near_by, call in calls:
        scalars = jnp.stack([x for _, _, pair in call for x in pair]).astype(jnp.int32)
        message = meet(scalars, near_by, [j for j, _, _ in call], [m for _, m, _ in call], message, exp_dev)
    rows_of = [[2 * z + s for z in range(length)] for s in range(2)]
    got = lax.all_to_all(message, "ep", split_axis=0, concat_axis=0, tiled=True, axis_index_groups=rows_of)
    late = last_dots(out_grad, other[length - 1], marks_at(place, place)[1], exp_dev)

    tokens, _ = lax.optimization_barrier((tokens, block))
    logits = lax.dot_general(router_weight, tokens, (((0,), (1,)), ((), ())), preferred_element_type=F32)
    logits = logits + router_bias[:, None]
    probability = jax.nn.softmax(logits, axis=0)
    mix = jax.nn.softmax(jnp.where(named, logits, -jnp.inf), axis=0)
    share_of = counts / (token_total * chosen)
    push = (balance_scale[0] * experts * share_of)[:, None]
    spread = probability * (push - jnp.sum(probability * push, axis=0, keepdims=True))
    prob_sums = jnp.sum(probability, axis=1)[None]

    spot = jnp.stack([side, place]).astype(jnp.int32)
    logit_grad, sent = finish(spot, got, late, mix, spread, prob_sums, tokens, dp, exp_dev)
    token_grad = lax.dot_general(
        logit_grad, router_weight, (((0,), (1,)), ((), ())), preferred_element_type=F32
    ).astype(BF16)
    summed = jnp.sum(lax.all_to_all(sent, ("ep", "dp"), split_axis=0, concat_axis=0, tiled=True), axis=0)
    piece = width // dp
    weight_grad = summed[:, :piece].T / math.sqrt(token_total)
    balance_loss = (experts * jnp.sum(share_of * (summed[0, piece:piece + experts] / token_total))).reshape(1)
    return (token_grad, weight_grad, balance_loss)


def solution(mesh):
    placed = (
        P(("ep", "dp"), None),
        P(("ep", "dp"), None),
        P(("ep", "dp"), None),
        P("dp", "ep", None, None, None),
        P(),
        P(),
        P(),
    )
    return jax.shard_map(
        on_device,
        mesh=mesh,
        in_specs=placed,
        out_specs=(P(("ep", "dp"), None), P("dp", "ep"), P()),
        check_vma=False,
    )
```

```python
import math

import jax
import jax.numpy as jnp
from jax import lax
from jax.experimental import pallas as pl
from jax.experimental.pallas import tpu as pltpu
from jax.sharding import PartitionSpec as P


F32, BF16 = jnp.float32, jnp.bfloat16


NT = (((1,), (1,)), ((), ()))
ANYWHERE = pl.BlockSpec(memory_space=pl.ANY)
SCALARS = pl.BlockSpec(memory_space=pltpu.SMEM)
LOCAL = pl.BlockSpec(memory_space=pltpu.VMEM)


def spot(length):
    me = lax.axis_index("ep")
    side, place = lax.rem(me, 2), lax.div(me, 2)
    return side, place, place < length - length // 2


def source_at(length, n):
    _, place, low = spot(length)
    ahead = place + jnp.where(low, length - 1 - n, n + 1)
    return jnp.where(ahead >= length, ahead - length, ahead)


def split_rows(table, wanted, ep):
    total, width = table.shape
    count, entries = len(wanted), total // ep
    rows = 16 if entries % 16 == 0 else entries
    block_in, parts = rows * ep, entries // rows
    group = max(g for g in (1, 2, 3) if parts % g == 0)

    def body(x_ref, *refs):
        outs, sel_ref = refs[:count], refs[count]

        @pl.when(pl.program_id(0) == 0)
        def _():
            side, _, _ = spot(ep // 2)
            row = lax.broadcasted_iota(jnp.int32, (rows, block_in), 0)
            column = lax.broadcasted_iota(jnp.int32, (rows, block_in), 1)
            for k, (n, across) in enumerate(wanted):
                source = 2 * source_at(ep // 2, n) + (1 - side if across else side)
                sel_ref[k * rows:(k + 1) * rows, :] = (column == row * ep + source).astype(F32).astype(BF16)

        for k in range(group):
            x = x_ref[k * block_in:(k + 1) * block_in, :]
            y = jnp.dot(sel_ref[...], x, preferred_element_type=F32).astype(BF16)
            for c in range(count):
                outs[c][k * rows:(k + 1) * rows, :] = y[c * rows:(c + 1) * rows]

    return pl.pallas_call(
        body,
        grid=(parts // group,),
        in_specs=[pl.BlockSpec((group * block_in, width), lambda i: (i, 0))],
        out_specs=[pl.BlockSpec((group * rows, width), lambda i: (i, 0))] * count,
        out_shape=[jax.ShapeDtypeStruct((entries, width), BF16)] * count,
        scratch_shapes=[pltpu.VMEM((count * rows, block_in), BF16)],
        cost_estimate=pl.CostEstimate(
            flops=2 * count * rows * block_in * width * parts, bytes_accessed=3 * total * width, transcendentals=0
        ),
        name="split_rows",
    )(table)


def slot_marks(chosen, ep, exp_dev):
    tok = chosen.shape[1]
    experts = ep * exp_dev

    def body(chosen_ref, out_ref):
        ids = lax.broadcasted_iota(jnp.int32, (experts, tok), 0)
        named = jnp.zeros((experts, tok), jnp.bool_)
        for k in range(chosen.shape[0]):
            named = named | (ids == chosen_ref[k:k + 1, :])
        earlier = lax.broadcasted_iota(jnp.int32, (tok, tok), 0) < lax.broadcasted_iota(jnp.int32, (tok, tok), 1)
        before = jnp.dot(
            named.astype(F32).astype(BF16), earlier.astype(F32).astype(BF16), preferred_element_type=F32
        )
        marks = jnp.where(named, before.astype(jnp.int32), -1)
        for j in range(ep):
            out_ref[:, j] = jnp.broadcast_to(marks[None, j * exp_dev:(j + 1) * exp_dev], (ep, exp_dev, tok))

    return pl.pallas_call(
        body,
        in_specs=[LOCAL],
        out_specs=LOCAL,
        out_shape=jax.ShapeDtypeStruct((ep, ep, exp_dev, tok), jnp.int32),
        cost_estimate=pl.CostEstimate(flops=2 * experts * tok * tok, bytes_accessed=4 * ep * experts * tok, transcendentals=0),
        name="slot_marks",
    )(chosen)


def router(weight, tokens, bias, marks):
    experts, tok = weight.shape[0], tokens.shape[0]

    def body(weight_ref, tokens_ref, bias_ref, marks_ref, probability_ref, mix_ref, sums_ref):
        logits = lax.dot_general(weight_ref[...], tokens_ref[...], NT, preferred_element_type=F32) + bias_ref[...]
        powers = jnp.exp(logits - jnp.max(logits, axis=0, keepdims=True))
        probability = powers / jnp.sum(powers, axis=0, keepdims=True)
        probability_ref[...] = probability
        named = jnp.concatenate([marks_ref[j] for j in range(marks.shape[0])], axis=0) >= 0
        best = jnp.max(jnp.where(named, logits, -jnp.inf), axis=0, keepdims=True)
        powers = jnp.where(named, jnp.exp(jnp.where(named, logits, best) - best), 0.0)
        mix_ref[...] = powers / jnp.sum(powers, axis=0, keepdims=True)
        square = (experts, experts)
        same = lax.broadcasted_iota(jnp.int32, square, 0) == lax.broadcasted_iota(jnp.int32, square, 1)
        sums = jnp.where(same, jnp.sum(probability, axis=1, keepdims=True), 0.0)
        sums_ref[...] = jnp.sum(sums, axis=0, keepdims=True)

    return pl.pallas_call(
        body,
        in_specs=[LOCAL] * 4,
        out_specs=[LOCAL] * 3,
        out_shape=[jax.ShapeDtypeStruct((experts, tok), F32)] * 2 + [jax.ShapeDtypeStruct((1, experts), F32)],
        cost_estimate=pl.CostEstimate(
            flops=2 * experts * tok * weight.shape[1], bytes_accessed=2 * (weight.size + tokens.size), transcendentals=2 * experts * tok
        ),
        name="router",
    )(weight, tokens, bias, marks)


def slot_dots(rows, block, marks, exp_dev, put):
    kinds, count, width = rows.shape
    tok, cap = block.shape[0], count // exp_dev
    if count % 16 == 0:
        full = lax.dot_general(rows[...].reshape(kinds * count, width), block[...], NT, preferred_element_type=F32)
        full = [full[k * count:(k + 1) * count] for k in range(kinds)]
    else:
        full = [lax.dot_general(rows[k], block[...], NT, preferred_element_type=F32) for k in range(kinds)]
    slots = lax.broadcasted_iota(jnp.int32, (cap, tok), 0)
    for kind, mark in enumerate(marks):
        for e in range(exp_dev):
            part = jnp.where(slots == mark[e:e + 1], full[kind][e * cap:(e + 1) * cap], 0.0)
            put(kind, e, jnp.sum(part, axis=0, keepdims=True))


def meet(blocks, jobs, marks, message, exp_dev):
    tok, width = blocks[0].shape
    length = message.shape[0]
    flat = [r for job in jobs for r in job[0]]
    count = flat[0].shape[0]
    most = max(len(job[0]) for job in jobs)
    first = [sum(len(job[0]) for job in jobs[:n]) for n in range(len(jobs))]

    def body(*refs):
        block_refs, refs = refs[:len(blocks)], refs[len(blocks):]
        row_refs, refs = refs[:len(flat)], refs[len(flat):]
        marks_ref, in_ref, out_ref, held, rows_held, block_sem, row_sem = refs
        side = spot(length)[0]
        plans = [job[2]() for job in jobs]

        def usable(n):
            return (plans[n][2] >= 0) & (plans[n][2] < len(blocks))

        def rows_copy(n, k):
            return pltpu.make_async_copy(row_refs[first[n] + k], rows_held.at[n % 2, k], row_sem.at[n % 2, k])

        def start(n):
            for i, block in enumerate(block_refs):
                @pl.when(plans[n][2] == i)
                def _(block=block):
                    pltpu.make_async_copy(block, held.at[n % 2], block_sem.at[n % 2]).start()

            @pl.when(usable(n))
            def _():
                for k in range(len(jobs[n][0])):
                    rows_copy(n, k).start()

        start(0)
        out_ref[...] = in_ref[...]
        for n in range(len(jobs)):
            if n + 1 < len(jobs):
                start(n + 1)

            @pl.when(usable(n))
            def _(n=n):
                pltpu.make_async_copy(block_refs[0], held.at[n % 2], block_sem.at[n % 2]).wait()
                rows, kinds = jobs[n][:2]
                source, column, _ = plans[n]
                for k in range(len(rows)):
                    rows_copy(n, k).wait()

                def put(k, e, value):
                    line = jobs[n][3] + kinds[k] * exp_dev + e
                    out_ref[pl.ds(source, 1), line:line + 1, :] = value[None]

                each = [marks_ref[2 * source + side, 2 * column + (1 - side if kind else side)] for kind in kinds]
                slot_dots(rows_held.at[n % 2, pl.ds(0, len(rows))], held.at[n % 2], each, exp_dev, put)

    return pl.pallas_call(
        body,
        in_specs=[ANYWHERE] * (len(blocks) + len(flat)) + [LOCAL] * 2,
        out_specs=LOCAL,
        out_shape=jax.ShapeDtypeStruct(message.shape, F32),
        input_output_aliases={1 + len(blocks) + len(flat): 0},
        scratch_shapes=[
            pltpu.VMEM((2, tok, width), BF16),
            pltpu.VMEM((2, most, count, width), BF16),
            pltpu.SemaphoreType.DMA((2,)),
            pltpu.SemaphoreType.DMA((2, most)),
        ],
        cost_estimate=pl.CostEstimate(
            flops=2 * len(flat) * tok * count * width, bytes_accessed=4 * len(flat) * count * width, transcendentals=0
        ),
        name="meet",
    )(*blocks, *flat, marks, message)


def last_dots(block, rows, marks, exp_dev):
    tok, length = block.shape[0], marks.shape[0] // 2

    def body(block_ref, rows_ref, marks_ref, out_ref):
        side, place, _ = spot(length)

        def put(kind, e, value):
            out_ref[e:e + 1, :] = value

        mark = marks_ref[2 * place + side, 2 * place + 1 - side]
        slot_dots(rows_ref, block_ref, [mark], exp_dev, put)

    return pl.pallas_call(
        body,
        in_specs=[LOCAL] * 3,
        out_specs=LOCAL,
        out_shape=jax.ShapeDtypeStruct((exp_dev, tok), F32),
        cost_estimate=pl.CostEstimate(
            flops=2 * tok * rows.size, bytes_accessed=2 * (block.size + rows.size), transcendentals=0
        ),
        name="last_dots",
    )(block, rows[None], marks)


def finish(got, late, mix, probability, counts, scale, prob_sums, tokens, dp, exp_dev, share):
    experts, tok = mix.shape
    length, width = got.shape[0], tokens.shape[1]
    ep, piece = 2 * length, width // dp
    far = got.shape[1] // (2 * exp_dev) - 1
    lanes = -(-(piece + experts) // 128) * 128

    def body(scale_ref, got_ref, late_ref, mix_ref, prob_ref, counts_ref, sums_ref, tokens_ref, grad_ref, sent_ref, dots_ref):
        side, place, _ = spot(length)
        square = (experts, experts)
        same = lax.broadcasted_iota(jnp.int32, square, 0) == lax.broadcasted_iota(jnp.int32, square, 1)
        total = jnp.sum(counts_ref[...], axis=0, keepdims=True) * share
        push = scale_ref[0] * experts * jnp.sum(jnp.where(same, total, 0.0), axis=1, keepdims=True)
        probability = prob_ref[...]
        spread = probability * (push - jnp.sum(probability * push, axis=0, keepdims=True))
        for c in range(length):
            for kind in range(2):
                value = got_ref[c, kind * exp_dev:(kind + 1) * exp_dev, :]
                for i in range(1, far + 1):
                    line = (2 * i + kind) * exp_dev
                    if c - i >= 0:
                        value += jnp.where(c - i > place, got_ref[c - i, line:line + exp_dev, :], 0.0)
                    if c + i < length:
                        value += jnp.where(c + i < place, got_ref[c + i, line:line + exp_dev, :], 0.0)
                if kind:
                    value += jnp.where(c == place, late_ref[...], 0.0)
                at = 2 * c + jnp.where(side == kind, 0, 1)
                dots_ref[pl.ds(at, 1), :, :] = value[None]
        dots = jnp.concatenate([dots_ref[j] for j in range(ep)], axis=0)
        mixed = mix_ref[...] * dots
        grad = (spread + (mixed - mix_ref[...] * jnp.sum(mixed, axis=0, keepdims=True))).astype(BF16)
        grad_ref[...] = grad
        term = jnp.dot(grad, tokens_ref[...], preferred_element_type=F32)
        for d in range(dp):
            part = term[:, d * piece:(d + 1) * piece]
            for j in range(ep):
                sent_ref[j * dp + d, :, :piece] = part[j * exp_dev:(j + 1) * exp_dev]
        sums = jnp.broadcast_to(sums_ref[...][None], (ep * dp, exp_dev, experts))
        sent_ref[:, :, piece:piece + experts] = sums
        if lanes > piece + experts:
            sent_ref[:, :, piece + experts:] = jnp.zeros((ep * dp, exp_dev, lanes - piece - experts), F32)

    return pl.pallas_call(
        body,
        in_specs=[SCALARS] + [LOCAL] * 7,
        out_specs=[LOCAL] * 2,
        out_shape=[
            jax.ShapeDtypeStruct((experts, tok), BF16),
            jax.ShapeDtypeStruct((ep * dp, exp_dev, lanes), F32),
        ],
        scratch_shapes=[pltpu.VMEM((ep, exp_dev, tok), F32)],
        cost_estimate=pl.CostEstimate(
            flops=2 * experts * tok * width, bytes_accessed=2 * tok * width + 4 * experts * width, transcendentals=0
        ),
        name="finish",
    )(scale, got, late, mix, probability, counts, prob_sums, tokens)


def on_device(tokens, out_grad, indices, expert_rows, router_weight, router_bias, balance_scale):
    tok, width = tokens.shape
    experts = router_weight.shape[1]
    exp_dev, capacity = expert_rows.shape[1], expert_rows.shape[3]
    ep, dp = lax.axis_size("ep"), lax.axis_size("dp")
    token_total = tok * ep * dp
    length = ep // 2
    reach = length // 2
    far = length - 1 - reach

    entries = exp_dev * capacity
    table = expert_rows.transpose(0, 1, 3, 2, 4).reshape(entries * ep, width)
    cross = [(j, j ^ 1) for j in range(ep)]
    leaving = list(split_rows(table, [(0, True)], ep))
    block, table, leaving[0] = lax.optimization_barrier((out_grad, table, leaving[0]))
    rest = list(split_rows(table, [(n, True) for n in range(1, length)] + [(n, False) for n in range(length)], ep))
    leaving, own = leaving + rest[:length - 1], rest[length - 1:]
    other = []
    for rows in leaving:
        other.append(lax.ppermute(rows, "ep", cross))

    def shift(x, *moves):
        pairs = [(z, to) for valid, by in moves for z in range(length) for to in [z + by] if valid(z) and 0 <= to < length]
        return lax.ppermute(x, "ep", [(2 * z + s, 2 * to + s) for z, to in pairs for s in range(2)])

    below, above = [block], [block]
    for hop in range(reach):
        below.append(shift(below[-1], (lambda z: z >= hop, 1)))
        above.append(shift(above[-1], (lambda z: z + hop < length, -1)))
    blocks = below[:0:-1] + [block] + above[1:]

    guests = []
    for i in range(1, far + 1):
        d = reach + i
        moves = ((lambda z: z + d < length, i), (lambda z: z - d >= 0, -i))
        guests.append([])
        for rows in (own, other):
            guests[-1].append(shift(rows[length - 1 - d], *moves))

    chosen, _ = lax.optimization_barrier((indices.T, rest[0]))
    mine = slot_marks(chosen, ep, exp_dev)
    marks = lax.all_to_all(mine, "ep", split_axis=0, concat_axis=0, tiled=True)
    counts = jnp.sum((marks >= 0).astype(F32), axis=(0, 3)).reshape(1, experts)
    counts = lax.all_to_all(jnp.broadcast_to(counts, (dp, experts)), "dp", split_axis=0, concat_axis=0, tiled=True)

    tokens, _ = lax.optimization_barrier((tokens, rest[0]))
    probability, mix, prob_sums = router(router_weight.T, tokens, router_bias[:, None], mine[0])

    def job(n, kinds, hops):
        def plan():
            _, place, _ = spot(length)
            source = source_at(length, n)
            return source, place, source - place + hops

        return [(own, other)[kind][n] for kind in kinds], kinds, plan, 0

    def guest_job(i):
        def plan():
            _, place, low = spot(length)
            column = place + jnp.where(low, -i, i)
            source = place + jnp.where(low, reach, -reach)
            there = (column >= 0) & (column < length) & (source >= 0) & (source < length)
            which = jnp.where(there, jnp.where(low, 1, 0), -1)
            return jnp.clip(source, 0, length - 1), jnp.clip(column, 0, length - 1), which

        return guests[i - 1], (0, 1), plan, 2 * i * exp_dev

    message = jnp.zeros((length, 2 * exp_dev * (1 + far), tok), F32)
    near = {0: (0, 1), length - 2: (0,), length - 1: (0,)}
    calls = [(blocks[reach - 1:reach + 2], [job(n, kinds, 1) for n, kinds in near.items()])]
    middle = [job(n, (0, 1), reach) for n in range(1, length - 2)]
    calls.append((blocks, middle + [job(length - 2, (1,), reach)]))
    if far:
        calls.append((blocks[::2 * reach], [guest_job(i) for i in range(1, far + 1)]))
    for near_by, jobs in calls:
        message = meet(near_by, jobs, marks, message, exp_dev)
    rows_of = [[2 * z + s for z in range(length)] for s in range(2)]
    got = lax.all_to_all(message, "ep", split_axis=0, concat_axis=0, tiled=True, axis_index_groups=rows_of)
    late = last_dots(out_grad, other[length - 1], marks, exp_dev)

    share = 1.0 / (token_total * indices.shape[1])
    logit_grad, sent = finish(
        got, late, mix, probability, counts, balance_scale, prob_sums, tokens, dp, exp_dev, share
    )
    token_grad = lax.dot_general(
        logit_grad, router_weight, (((0,), (1,)), ((), ())), preferred_element_type=F32
    ).astype(BF16)
    summed = jnp.sum(lax.all_to_all(sent, ("ep", "dp"), split_axis=0, concat_axis=0, tiled=True), axis=0)
    share_of = jnp.sum(counts, axis=0) * share
    piece = width // dp
    weight_grad = summed[:, :piece].T / math.sqrt(token_total)
    balance_loss = (experts * jnp.sum(share_of * (summed[0, piece:piece + experts] / token_total))).reshape(1)
    return (token_grad, weight_grad, balance_loss)


def solution(mesh):
    placed = (
        P(("ep", "dp"), None),
        P(("ep", "dp"), None),
        P(("ep", "dp"), None),
        P("dp", "ep", None, None, None),
        P(),
        P(),
        P(),
    )

    return jax.shard_map(
        on_device,
        mesh=mesh,
        in_specs=placed,
        out_specs=(P(("ep", "dp"), None), P("dp", "ep"), P()),
        check_vma=False,
    )
```

```python
import math

import jax
import jax.numpy as jnp
from jax import lax
from jax.experimental import pallas as pl
from jax.experimental.pallas import tpu as pltpu
from jax.sharding import PartitionSpec as P


F32, BF16 = jnp.float32, jnp.bfloat16


NT = (((1,), (1,)), ((), ()))
ANYWHERE = pl.BlockSpec(memory_space=pl.ANY)
SCALARS = pl.BlockSpec(memory_space=pltpu.SMEM)
LOCAL = pl.BlockSpec(memory_space=pltpu.VMEM)


def spot(length):
    me = lax.axis_index("ep")
    side, place = lax.rem(me, 2), lax.div(me, 2)
    return side, place, place < length - length // 2


def source_at(length, n):
    _, place, low = spot(length)
    ahead = place + jnp.where(low, length - 1 - n, n + 1)
    return jnp.where(ahead >= length, ahead - length, ahead)


def split_rows(table, wanted, ep):
    total, width = table.shape
    count, entries = len(wanted), total // ep
    rows = 16 if entries % 16 == 0 else entries
    block_in, parts = rows * ep, entries // rows
    group = max(g for g in (1, 2, 3) if parts % g == 0)

    def body(x_ref, *refs):
        outs, sel_ref = refs[:count], refs[count]

        @pl.when(pl.program_id(0) == 0)
        def _():
            side, _, _ = spot(ep // 2)
            row = lax.broadcasted_iota(jnp.int32, (rows, block_in), 0)
            column = lax.broadcasted_iota(jnp.int32, (rows, block_in), 1)
            for k, (n, across) in enumerate(wanted):
                source = 2 * source_at(ep // 2, n) + (1 - side if across else side)
                sel_ref[k * rows:(k + 1) * rows, :] = (column == row * ep + source).astype(F32).astype(BF16)

        for k in range(group):
            x = x_ref[k * block_in:(k + 1) * block_in, :]
            y = jnp.dot(sel_ref[...], x, preferred_element_type=F32).astype(BF16)
            for c in range(count):
                outs[c][k * rows:(k + 1) * rows, :] = y[c * rows:(c + 1) * rows]

    return pl.pallas_call(
        body,
        grid=(parts // group,),
        in_specs=[pl.BlockSpec((group * block_in, width), lambda i: (i, 0))],
        out_specs=[pl.BlockSpec((group * rows, width), lambda i: (i, 0))] * count,
        out_shape=[jax.ShapeDtypeStruct((entries, width), BF16)] * count,
        scratch_shapes=[pltpu.VMEM((count * rows, block_in), BF16)],
        cost_estimate=pl.CostEstimate(
            flops=2 * count * rows * block_in * width * parts, bytes_accessed=3 * total * width, transcendentals=0
        ),
        name="split_rows",
    )(table)


def slot_marks(chosen, ep, exp_dev):
    tok = chosen.shape[1]
    experts = ep * exp_dev

    def body(chosen_ref, out_ref):
        ids = lax.broadcasted_iota(jnp.int32, (experts, tok), 0)
        named = jnp.zeros((experts, tok), jnp.bool_)
        for k in range(chosen.shape[0]):
            named = named | (ids == chosen_ref[k:k + 1, :])
        earlier = lax.broadcasted_iota(jnp.int32, (tok, tok), 0) < lax.broadcasted_iota(jnp.int32, (tok, tok), 1)
        before = jnp.dot(
            named.astype(F32).astype(BF16), earlier.astype(F32).astype(BF16), preferred_element_type=F32
        )
        marks = jnp.where(named, before.astype(jnp.int32), -1)
        for j in range(ep):
            out_ref[:, j] = jnp.broadcast_to(marks[None, j * exp_dev:(j + 1) * exp_dev], (ep, exp_dev, tok))

    return pl.pallas_call(
        body,
        in_specs=[LOCAL],
        out_specs=LOCAL,
        out_shape=jax.ShapeDtypeStruct((ep, ep, exp_dev, tok), jnp.int32),
        cost_estimate=pl.CostEstimate(flops=2 * experts * tok * tok, bytes_accessed=4 * ep * experts * tok, transcendentals=0),
        name="slot_marks",
    )(chosen)


def router(weight, tokens, bias, marks):
    experts, tok = weight.shape[0], tokens.shape[0]

    def body(weight_ref, tokens_ref, bias_ref, marks_ref, probability_ref, mix_ref, sums_ref):
        logits = lax.dot_general(weight_ref[...], tokens_ref[...], NT, preferred_element_type=F32) + bias_ref[...]
        powers = jnp.exp(logits - jnp.max(logits, axis=0, keepdims=True))
        probability = powers / jnp.sum(powers, axis=0, keepdims=True)
        probability_ref[...] = probability
        named = jnp.concatenate([marks_ref[j] for j in range(marks.shape[0])], axis=0) >= 0
        best = jnp.max(jnp.where(named, logits, -jnp.inf), axis=0, keepdims=True)
        powers = jnp.where(named, jnp.exp(jnp.where(named, logits, best) - best), 0.0)
        mix_ref[...] = powers / jnp.sum(powers, axis=0, keepdims=True)
        square = (experts, experts)
        same = lax.broadcasted_iota(jnp.int32, square, 0) == lax.broadcasted_iota(jnp.int32, square, 1)
        sums = jnp.where(same, jnp.sum(probability, axis=1, keepdims=True), 0.0)
        sums_ref[...] = jnp.sum(sums, axis=0, keepdims=True)

    return pl.pallas_call(
        body,
        in_specs=[LOCAL] * 4,
        out_specs=[LOCAL] * 3,
        out_shape=[jax.ShapeDtypeStruct((experts, tok), F32)] * 2 + [jax.ShapeDtypeStruct((1, experts), F32)],
        cost_estimate=pl.CostEstimate(
            flops=2 * experts * tok * weight.shape[1], bytes_accessed=2 * (weight.size + tokens.size), transcendentals=2 * experts * tok
        ),
        name="router",
    )(weight, tokens, bias, marks)


def slot_dots(rows, block, marks, exp_dev, put):
    kinds, count, width = rows.shape
    tok, cap = block.shape[0], count // exp_dev
    if count % 16 == 0:
        full = lax.dot_general(rows[...].reshape(kinds * count, width), block[...], NT, preferred_element_type=F32)
        full = [full[k * count:(k + 1) * count] for k in range(kinds)]
    else:
        full = [lax.dot_general(rows[k], block[...], NT, preferred_element_type=F32) for k in range(kinds)]
    slots = lax.broadcasted_iota(jnp.int32, (cap, tok), 0)
    for kind, mark in enumerate(marks):
        for e in range(exp_dev):
            part = jnp.where(slots == mark[e:e + 1], full[kind][e * cap:(e + 1) * cap], 0.0)
            put(kind, e, jnp.sum(part, axis=0, keepdims=True))


def meet(blocks, jobs, marks, message, exp_dev):
    tok, width = blocks[0].shape
    length = marks.shape[0] // 2
    flat = [r for job in jobs for r in job[0]]
    count = flat[0].shape[0]
    most = max(len(job[0]) for job in jobs)
    first = [sum(len(job[0]) for job in jobs[:n]) for n in range(len(jobs))]

    def body(*refs):
        block_refs, refs = refs[:len(blocks)], refs[len(blocks):]
        row_refs, refs = refs[:len(flat)], refs[len(flat):]
        marks_ref, in_ref, out_ref, held, rows_held, block_sem, row_sem = refs
        side = spot(length)[0]
        plans = [job[2]() for job in jobs]

        def usable(n):
            return (plans[n][2] >= 0) & (plans[n][2] < len(blocks))

        def rows_copy(n, k):
            return pltpu.make_async_copy(row_refs[first[n] + k], rows_held.at[n % 2, k], row_sem.at[n % 2, k])

        def start(n):
            for i, block in enumerate(block_refs):
                @pl.when(plans[n][2] == i)
                def _(block=block):
                    pltpu.make_async_copy(block, held.at[n % 2], block_sem.at[n % 2]).start()

            @pl.when(usable(n))
            def _():
                for k in range(len(jobs[n][0])):
                    rows_copy(n, k).start()

        start(0)
        out_ref[...] = in_ref[...]
        for n in range(len(jobs)):
            if n + 1 < len(jobs):
                start(n + 1)

            @pl.when(usable(n))
            def _(n=n):
                pltpu.make_async_copy(block_refs[0], held.at[n % 2], block_sem.at[n % 2]).wait()
                rows, kinds = jobs[n][:2]
                source, column, _, target = plans[n]
                for k in range(len(rows)):
                    rows_copy(n, k).wait()

                def put(k, e, value):
                    line = jobs[n][3] + kinds[k] * exp_dev + e
                    out_ref[pl.ds(target, 1), line:line + 1, :] = value[None]

                each = [marks_ref[2 * source + side, 2 * column + (1 - side if kind else side)] for kind in kinds]
                slot_dots(rows_held.at[n % 2, pl.ds(0, len(rows))], held.at[n % 2], each, exp_dev, put)

    return pl.pallas_call(
        body,
        in_specs=[ANYWHERE] * (len(blocks) + len(flat)) + [LOCAL] * 2,
        out_specs=LOCAL,
        out_shape=jax.ShapeDtypeStruct(message.shape, F32),
        input_output_aliases={1 + len(blocks) + len(flat): 0},
        scratch_shapes=[
            pltpu.VMEM((2, tok, width), BF16),
            pltpu.VMEM((2, most, count, width), BF16),
            pltpu.SemaphoreType.DMA((2,)),
            pltpu.SemaphoreType.DMA((2, most)),
        ],
        cost_estimate=pl.CostEstimate(
            flops=2 * len(flat) * tok * count * width, bytes_accessed=4 * len(flat) * count * width, transcendentals=0
        ),
        name="meet",
    )(*blocks, *flat, marks, message)


def last_dots(block, rows, marks, exp_dev):
    tok, length = block.shape[0], marks.shape[0] // 2

    def body(block_ref, rows_ref, marks_ref, out_ref):
        side, place, _ = spot(length)

        def put(kind, e, value):
            out_ref[e:e + 1, :] = value

        mark = marks_ref[2 * place + side, 2 * place + 1 - side]
        slot_dots(rows_ref, block_ref, [mark], exp_dev, put)

    return pl.pallas_call(
        body,
        in_specs=[LOCAL] * 3,
        out_specs=LOCAL,
        out_shape=jax.ShapeDtypeStruct((exp_dev, tok), F32),
        cost_estimate=pl.CostEstimate(
            flops=2 * tok * rows.size, bytes_accessed=2 * (block.size + rows.size), transcendentals=0
        ),
        name="last_dots",
    )(block, rows[None], marks)


def finish(got, guest, late, mix, probability, counts, scale, prob_sums, tokens, dp, exp_dev, share):
    experts, tok = mix.shape
    length, width = got.shape[0], tokens.shape[1]
    ep, piece = 2 * length, width // dp
    reach, far = length // 2, guest.shape[1] // (2 * exp_dev)
    lanes = -(-(piece + experts) // 128) * 128

    def body(scale_ref, got_ref, guest_ref, late_ref, mix_ref, prob_ref, counts_ref, sums_ref, tokens_ref, grad_ref, sent_ref, dots_ref):
        side, place, _ = spot(length)
        square = (experts, experts)
        same = lax.broadcasted_iota(jnp.int32, square, 0) == lax.broadcasted_iota(jnp.int32, square, 1)
        total = jnp.sum(counts_ref[...], axis=0, keepdims=True) * share
        push = scale_ref[0] * experts * jnp.sum(jnp.where(same, total, 0.0), axis=1, keepdims=True)
        probability = prob_ref[...]
        spread = probability * (push - jnp.sum(probability * push, axis=0, keepdims=True))
        for c in range(length):
            for kind in range(2):
                value = got_ref[c, kind * exp_dev:(kind + 1) * exp_dev, :]
                for i in range(1, far + 1):
                    line = (2 * (i - 1) + kind) * exp_dev
                    column = place + jnp.where(place < reach, reach + i, -reach - i)
                    value += jnp.where(c == column, guest_ref[0, line:line + exp_dev, :], 0.0)
                if kind:
                    value += jnp.where(c == place, late_ref[...], 0.0)
                at = 2 * c + jnp.where(side == kind, 0, 1)
                dots_ref[pl.ds(at, 1), :, :] = value[None]
        dots = jnp.concatenate([dots_ref[j] for j in range(ep)], axis=0)
        mixed = mix_ref[...] * dots
        grad = (spread + (mixed - mix_ref[...] * jnp.sum(mixed, axis=0, keepdims=True))).astype(BF16)
        grad_ref[...] = grad
        term = jnp.dot(grad, tokens_ref[...], preferred_element_type=F32)
        for d in range(dp):
            part = term[:, d * piece:(d + 1) * piece]
            for j in range(ep):
                sent_ref[j * dp + d, :, :piece] = part[j * exp_dev:(j + 1) * exp_dev]
        sums = jnp.broadcast_to(sums_ref[...][None], (ep * dp, exp_dev, experts))
        sent_ref[:, :, piece:piece + experts] = sums
        if lanes > piece + experts:
            sent_ref[:, :, piece + experts:] = jnp.zeros((ep * dp, exp_dev, lanes - piece - experts), F32)

    return pl.pallas_call(
        body,
        in_specs=[SCALARS] + [LOCAL] * 8,
        out_specs=[LOCAL] * 2,
        out_shape=[
            jax.ShapeDtypeStruct((experts, tok), BF16),
            jax.ShapeDtypeStruct((ep * dp, exp_dev, lanes), F32),
        ],
        scratch_shapes=[pltpu.VMEM((ep, exp_dev, tok), F32)],
        cost_estimate=pl.CostEstimate(
            flops=2 * experts * tok * width, bytes_accessed=2 * tok * width + 4 * experts * width, transcendentals=0
        ),
        name="finish",
    )(scale, got, guest, late, mix, probability, counts, prob_sums, tokens)


def on_device(tokens, out_grad, indices, expert_rows, router_weight, router_bias, balance_scale):
    tok, width = tokens.shape
    experts = router_weight.shape[1]
    exp_dev, capacity = expert_rows.shape[1], expert_rows.shape[3]
    ep, dp = lax.axis_size("ep"), lax.axis_size("dp")
    token_total = tok * ep * dp
    assert ep % 4 == 0
    length = ep // 2
    reach = length // 2
    far = length - 1 - reach

    entries = exp_dev * capacity
    table = expert_rows.transpose(0, 1, 3, 2, 4).reshape(entries * ep, width)
    cross = [(j, j ^ 1) for j in range(ep)]
    leaving = list(split_rows(table, [(0, True)], ep))
    table, leaving[0] = lax.optimization_barrier((table, leaving[0]))
    block = out_grad
    rest = list(split_rows(table, [(n, True) for n in range(1, length)] + [(n, False) for n in range(length)], ep))
    leaving, own = leaving + rest[:length - 1], rest[length - 1:]
    other = []
    for rows in leaving:
        other.append(lax.ppermute(rows, "ep", cross))

    def shift(x, *moves):
        pairs = [(z, to) for valid, by in moves for z in range(length) for to in [z + by] if valid(z) and 0 <= to < length]
        return lax.ppermute(x, "ep", [(2 * z + s, 2 * to + s) for z, to in pairs for s in range(2)])

    below, above = [block], [block]
    for hop in range(reach):
        below.append(shift(below[-1], (lambda z: z >= hop, 1)))
        above.append(shift(above[-1], (lambda z: z + hop < length, -1)))
    blocks = below[:0:-1] + [block] + above[1:]

    guests = []
    for i in range(1, far + 1):
        d = reach + i
        moves = ((lambda z: z + d < length, i), (lambda z: z - d >= 0, -i))
        guests.append([])
        for rows in (own, other):
            guests[-1].append(shift(rows[length - 1 - d], *moves))

    chosen, _ = lax.optimization_barrier((indices.T, rest[0]))
    mine = slot_marks(chosen, ep, exp_dev)
    marks = lax.all_to_all(mine, "ep", split_axis=0, concat_axis=0, tiled=True)
    counts = jnp.sum((marks >= 0).astype(F32), axis=(0, 3)).reshape(1, experts)
    counts = lax.all_to_all(jnp.broadcast_to(counts, (dp, experts)), "dp", split_axis=0, concat_axis=0, tiled=True)

    tokens, _ = lax.optimization_barrier((tokens, rest[0]))
    probability, mix, prob_sums = router(router_weight.T, tokens, router_bias[:, None], mine[0])

    def job(n, kinds, hops):
        def plan():
            _, place, _ = spot(length)
            source = source_at(length, n)
            return source, place, source - place + hops, source

        return [(own, other)[kind][n] for kind in kinds], kinds, plan, 0

    def guest_job(i, kind):
        def plan():
            _, place, low = spot(length)
            column = place + jnp.where(low, -i, i)
            source = place + jnp.where(low, reach, -reach)
            there = (column >= 0) & (column < length)
            which = jnp.where(there, jnp.where(low, 1, 0), -1)
            return source, jnp.clip(column, 0, length - 1), which, 0

        return [guests[i - 1][kind]], (kind,), plan, 2 * (i - 1) * exp_dev

    message = jnp.zeros((length, 2 * exp_dev, tok), F32)
    near = [job(0, (0, 1), 1), job(length - 2, (0,), 1), job(length - 1, (0,), 1)]
    message = meet(blocks[reach - 1:reach + 2], near, marks, message, exp_dev)
    message = meet(blocks, [job(n, (0, 1), reach) for n in range(1, length - 2)], marks, message, exp_dev)
    message = meet(blocks[reach - 1:reach + 2], [job(length - 2, (1,), 1)], marks, message, exp_dev)
    rows_of = [[2 * z + s for z in range(length)] for s in range(2)]
    got = lax.all_to_all(message, "ep", split_axis=0, concat_axis=0, tiled=True, axis_index_groups=rows_of)
    guest = jnp.zeros((1, 2 * exp_dev * far, tok), F32)
    for kind in range(2):
        guest = meet(blocks[::2 * reach], [guest_job(i, kind) for i in range(1, far + 1)], marks, guest, exp_dev)
    guest = shift(guest, (lambda z: 0 < z < reach, reach), (lambda z: reach <= z < length - 1, -reach))
    late = last_dots(out_grad, other[length - 1], marks, exp_dev)

    share = 1.0 / (token_total * indices.shape[1])
    logit_grad, sent = finish(
        got, guest, late, mix, probability, counts, balance_scale, prob_sums, tokens, dp, exp_dev, share
    )
    token_grad = lax.dot_general(
        logit_grad, router_weight, (((0,), (1,)), ((), ())), preferred_element_type=F32
    ).astype(BF16)
    summed = jnp.sum(lax.all_to_all(sent, ("ep", "dp"), split_axis=0, concat_axis=0, tiled=True), axis=0)
    share_of = jnp.sum(counts, axis=0) * share
    piece = width // dp
    weight_grad = summed[:, :piece].T / math.sqrt(token_total)
    balance_loss = (experts * jnp.sum(share_of * (summed[0, piece:piece + experts] / token_total))).reshape(1)
    return (token_grad, weight_grad, balance_loss)


def solution(mesh):
    placed = (
        P(("ep", "dp"), None),
        P(("ep", "dp"), None),
        P(("ep", "dp"), None),
        P("dp", "ep", None, None, None),
        P(),
        P(),
        P(),
    )

    return jax.shard_map(
        on_device,
        mesh=mesh,
        in_specs=placed,
        out_specs=(P(("ep", "dp"), None), P("dp", "ep"), P()),
        check_vma=False,
    )
```

```python
import math

import jax
import jax.numpy as jnp
from jax import lax
from jax.experimental import pallas as pl
from jax.experimental.pallas import tpu as pltpu
from jax.sharding import PartitionSpec as P


F32, BF16 = jnp.float32, jnp.bfloat16


NT = (((1,), (1,)), ((), ()))
ANYWHERE = pl.BlockSpec(memory_space=pl.ANY)
SCALARS = pl.BlockSpec(memory_space=pltpu.SMEM)
LOCAL = pl.BlockSpec(memory_space=pltpu.VMEM)


def spot(length):
    me = lax.axis_index("ep")
    side, place = lax.rem(me, 2), lax.div(me, 2)
    return side, place, place < length - length // 2


def source_at(length, n):
    _, place, low = spot(length)
    ahead = place + jnp.where(low, length - 1 - n, n + 1)
    return jnp.where(ahead >= length, ahead - length, ahead)


def split_rows(table, wanted, ep):
    total, width = table.shape
    count, entries = len(wanted), total // ep
    rows = 16 if entries % 16 == 0 else entries
    block_in, parts = rows * ep, entries // rows
    group = max(g for g in (1, 2, 3) if parts % g == 0)

    def body(x_ref, *refs):
        outs, sel_ref = refs[:count], refs[count]

        @pl.when(pl.program_id(0) == 0)
        def _():
            side, _, _ = spot(ep // 2)
            row = lax.broadcasted_iota(jnp.int32, (rows, block_in), 0)
            column = lax.broadcasted_iota(jnp.int32, (rows, block_in), 1)
            for k, (n, across) in enumerate(wanted):
                source = 2 * source_at(ep // 2, n) + (1 - side if across else side)
                sel_ref[k * rows:(k + 1) * rows, :] = (column == row * ep + source).astype(F32).astype(BF16)

        for k in range(group):
            x = x_ref[k * block_in:(k + 1) * block_in, :]
            y = jnp.dot(sel_ref[...], x, preferred_element_type=F32).astype(BF16)
            for c in range(count):
                outs[c][k * rows:(k + 1) * rows, :] = y[c * rows:(c + 1) * rows]

    return pl.pallas_call(
        body,
        grid=(parts // group,),
        in_specs=[pl.BlockSpec((group * block_in, width), lambda i: (i, 0))],
        out_specs=[pl.BlockSpec((group * rows, width), lambda i: (i, 0))] * count,
        out_shape=[jax.ShapeDtypeStruct((entries, width), BF16)] * count,
        scratch_shapes=[pltpu.VMEM((count * rows, block_in), BF16)],
        cost_estimate=pl.CostEstimate(
            flops=2 * count * rows * block_in * width * parts, bytes_accessed=3 * total * width, transcendentals=0
        ),
        name="split_rows",
    )(table)


def slot_marks(chosen, ep, exp_dev):
    tok = chosen.shape[1]
    experts = ep * exp_dev

    def body(chosen_ref, out_ref):
        ids = lax.broadcasted_iota(jnp.int32, (experts, tok), 0)
        named = jnp.zeros((experts, tok), jnp.bool_)
        for k in range(chosen.shape[0]):
            named = named | (ids == chosen_ref[k:k + 1, :])
        earlier = lax.broadcasted_iota(jnp.int32, (tok, tok), 0) < lax.broadcasted_iota(jnp.int32, (tok, tok), 1)
        before = jnp.dot(
            named.astype(F32).astype(BF16), earlier.astype(F32).astype(BF16), preferred_element_type=F32
        )
        marks = jnp.where(named, before.astype(jnp.int32), -1)
        for j in range(ep):
            out_ref[:, j] = jnp.broadcast_to(marks[None, j * exp_dev:(j + 1) * exp_dev], (ep, exp_dev, tok))

    return pl.pallas_call(
        body,
        in_specs=[LOCAL],
        out_specs=LOCAL,
        out_shape=jax.ShapeDtypeStruct((ep, ep, exp_dev, tok), jnp.int32),
        cost_estimate=pl.CostEstimate(flops=2 * experts * tok * tok, bytes_accessed=4 * ep * experts * tok, transcendentals=0),
        name="slot_marks",
    )(chosen)


def router(weight, tokens, bias, marks):
    experts, tok = weight.shape[0], tokens.shape[0]

    def body(weight_ref, tokens_ref, bias_ref, marks_ref, probability_ref, mix_ref, sums_ref):
        logits = lax.dot_general(weight_ref[...], tokens_ref[...], NT, preferred_element_type=F32) + bias_ref[...]
        powers = jnp.exp(logits - jnp.max(logits, axis=0, keepdims=True))
        probability = powers / jnp.sum(powers, axis=0, keepdims=True)
        probability_ref[...] = probability
        named = jnp.concatenate([marks_ref[j] for j in range(marks.shape[0])], axis=0) >= 0
        best = jnp.max(jnp.where(named, logits, -jnp.inf), axis=0, keepdims=True)
        powers = jnp.where(named, jnp.exp(jnp.where(named, logits, best) - best), 0.0)
        mix_ref[...] = powers / jnp.sum(powers, axis=0, keepdims=True)
        square = (experts, experts)
        same = lax.broadcasted_iota(jnp.int32, square, 0) == lax.broadcasted_iota(jnp.int32, square, 1)
        sums = jnp.where(same, jnp.sum(probability, axis=1, keepdims=True), 0.0)
        sums_ref[...] = jnp.sum(sums, axis=0, keepdims=True)

    return pl.pallas_call(
        body,
        in_specs=[LOCAL] * 4,
        out_specs=[LOCAL] * 3,
        out_shape=[jax.ShapeDtypeStruct((experts, tok), F32)] * 2 + [jax.ShapeDtypeStruct((1, experts), F32)],
        cost_estimate=pl.CostEstimate(
            flops=2 * experts * tok * weight.shape[1], bytes_accessed=2 * (weight.size + tokens.size), transcendentals=2 * experts * tok
        ),
        name="router",
    )(weight, tokens, bias, marks)


def offsets(mark, exp_dev):
    begin, total = [], jnp.zeros((1, 1), jnp.int32)
    for e in range(exp_dev):
        begin.append(total)
        total = total + jnp.sum((mark[e:e + 1] >= 0).astype(jnp.int32), axis=1, keepdims=True)
    return begin + [total]


def pack_rows(chunks, places, marks, exp_dev, size):
    entries, width = chunks[0].shape
    length, cap = marks.shape[0] // 2, entries // exp_dev

    def body(*refs):
        chunk_refs, marks_ref, outs = refs[:len(chunks)], refs[len(chunks)], refs[len(chunks) + 1:]
        side, place, _ = spot(length)
        row = lax.broadcasted_iota(jnp.int32, (size, entries), 0)
        entry = lax.broadcasted_iota(jnp.int32, (size, entries), 1)
        for chunk, n, out in zip(chunk_refs, places, outs):
            mark = marks_ref[2 * source_at(length, n) + 1 - side, 2 * place + side]
            begin = offsets(mark, exp_dev)
            sel = jnp.zeros((size, entries), F32)
            for e in range(exp_dev):
                slot = entry - e * cap
                used = (slot >= 0) & (slot < begin[e + 1] - begin[e])
                sel = jnp.where(used & (row == begin[e] + slot), 1.0, sel)
            out[...] = jnp.dot(sel.astype(BF16), chunk[...], preferred_element_type=F32).astype(BF16)

    return pl.pallas_call(
        body,
        in_specs=[LOCAL] * (len(chunks) + 1),
        out_specs=[LOCAL] * len(chunks),
        out_shape=[jax.ShapeDtypeStruct((size, width), BF16)] * len(chunks),
        cost_estimate=pl.CostEstimate(
            flops=2 * len(chunks) * size * entries * width, bytes_accessed=4 * len(chunks) * entries * width, transcendentals=0
        ),
        name="pack_rows",
    )(*chunks, marks)


def slot_dots(rows, block, marks, exp_dev, entries, put):
    kinds, count, width = rows.shape
    cap = entries // exp_dev
    if count % 16 == 0:
        full = lax.dot_general(rows[...].reshape(kinds * count, width), block[...], NT, preferred_element_type=F32)
        full = [full[k * count:(k + 1) * count] for k in range(kinds)]
    else:
        full = [lax.dot_general(rows[k], block[...], NT, preferred_element_type=F32) for k in range(kinds)]
    for kind, mark in enumerate(marks):
        begin = offsets(mark, exp_dev)
        for e in range(exp_dev):
            at = mark[e:e + 1]
            part = full[kind][e * cap:(e + 1) * cap]
            if count != entries:
                at = jnp.where(at >= 0, at + begin[e], -1)
                part = full[kind]
            slots = lax.broadcasted_iota(jnp.int32, part.shape, 0)
            put(kind, e, jnp.sum(jnp.where(slots == at, part, 0.0), axis=0, keepdims=True))


def meet(blocks, jobs, marks, answers, exp_dev, entries):
    tok, width = blocks[0].shape
    length = marks.shape[0] // 2
    flat = [r for job in jobs for r in job[0]]
    most = max(len(job[0]) for job in jobs)
    first = [sum(len(job[0]) for job in jobs[:n]) for n in range(len(jobs))]

    def body(*refs):
        block_refs, refs = refs[:len(blocks)], refs[len(blocks):]
        row_refs, refs = refs[:len(flat)], refs[len(flat):]
        marks_ref, refs = refs[0], refs[1:]
        in_refs, refs = refs[:len(answers)], refs[len(answers):]
        out_refs, (held, rows_held, block_sem, row_sem) = refs[:len(answers)], refs[len(answers):]
        side = spot(length)[0]
        plans = [job[2]() for job in jobs]

        def usable(n):
            return (plans[n][2] >= 0) & (plans[n][2] < len(blocks))

        def rows_copy(n, k):
            source = row_refs[first[n] + k]
            to = rows_held.at[n % 2, k, pl.ds(0, source.shape[0])] if source.shape[0] != entries else rows_held.at[n % 2, k]
            return pltpu.make_async_copy(source, to, row_sem.at[n % 2, k])

        def start(n):
            for i, block in enumerate(block_refs):
                @pl.when(plans[n][2] == i)
                def _(block=block):
                    pltpu.make_async_copy(block, held.at[n % 2], block_sem.at[n % 2]).start()

            @pl.when(usable(n))
            def _():
                for k in range(len(jobs[n][0])):
                    rows_copy(n, k).start()

        start(0)
        for in_ref, out_ref in zip(in_refs, out_refs):
            out_ref[...] = in_ref[...]
        for n in range(len(jobs)):
            if n + 1 < len(jobs):
                start(n + 1)

            @pl.when(usable(n))
            def _(n=n):
                pltpu.make_async_copy(block_refs[0], held.at[n % 2], block_sem.at[n % 2]).wait()
                rows, kinds = jobs[n][:2]
                source, column, _, target = plans[n]
                for k in range(len(rows)):
                    rows_copy(n, k).wait()

                def put(k, e, value):
                    line = jobs[n][3] + kinds[k] * exp_dev + e
                    out_refs[jobs[n][4]][pl.ds(target, 1), line:line + 1, :] = value[None]

                each = [marks_ref[2 * source + side, 2 * column + (1 - side if kind else side)] for kind in kinds]
                count = rows[0].shape[0]
                lines = rows_held.at[n % 2, pl.ds(0, len(rows))]
                if count != entries:
                    lines = rows_held.at[n % 2, pl.ds(0, len(rows)), pl.ds(0, count)]
                slot_dots(lines, held.at[n % 2], each, exp_dev, entries, put)

    given = len(blocks) + len(flat) + 1
    return pl.pallas_call(
        body,
        in_specs=[ANYWHERE] * (given - 1) + [LOCAL] * (1 + len(answers)),
        out_specs=[LOCAL] * len(answers),
        out_shape=[jax.ShapeDtypeStruct(x.shape, F32) for x in answers],
        input_output_aliases={given + i: i for i in range(len(answers))},
        scratch_shapes=[
            pltpu.VMEM((2, tok, width), BF16),
            pltpu.VMEM((2, most, entries, width), BF16),
            pltpu.SemaphoreType.DMA((2,)),
            pltpu.SemaphoreType.DMA((2, most)),
        ],
        cost_estimate=pl.CostEstimate(
            flops=2 * len(flat) * tok * entries * width, bytes_accessed=4 * len(flat) * entries * width, transcendentals=0
        ),
        name="meet",
    )(*blocks, *flat, marks, *answers)


def last_dots(block, rows, marks, exp_dev, entries):
    tok, length = block.shape[0], marks.shape[0] // 2

    def body(block_ref, rows_ref, marks_ref, out_ref):
        side, place, _ = spot(length)

        def put(kind, e, value):
            out_ref[e:e + 1, :] = value

        mark = marks_ref[2 * place + side, 2 * place + 1 - side]
        slot_dots(rows_ref, block_ref, [mark], exp_dev, entries, put)

    return pl.pallas_call(
        body,
        in_specs=[LOCAL] * 3,
        out_specs=LOCAL,
        out_shape=jax.ShapeDtypeStruct((exp_dev, tok), F32),
        cost_estimate=pl.CostEstimate(
            flops=2 * tok * rows.size, bytes_accessed=2 * (block.size + rows.size), transcendentals=0
        ),
        name="last_dots",
    )(block, rows[None], marks)


def finish(got, guest, late, mix, probability, counts, scale, prob_sums, tokens, dp, exp_dev, share):
    experts, tok = mix.shape
    length, width = got.shape[0], tokens.shape[1]
    ep, piece = 2 * length, width // dp
    reach, far = length // 2, guest.shape[1] // (2 * exp_dev)
    lanes = -(-(piece + experts) // 128) * 128

    def body(scale_ref, got_ref, guest_ref, late_ref, mix_ref, prob_ref, counts_ref, sums_ref, tokens_ref, grad_ref, sent_ref, dots_ref):
        side, place, _ = spot(length)
        square = (experts, experts)
        same = lax.broadcasted_iota(jnp.int32, square, 0) == lax.broadcasted_iota(jnp.int32, square, 1)
        total = jnp.sum(counts_ref[...], axis=0, keepdims=True) * share
        push = scale_ref[0] * experts * jnp.sum(jnp.where(same, total, 0.0), axis=1, keepdims=True)
        probability = prob_ref[...]
        spread = probability * (push - jnp.sum(probability * push, axis=0, keepdims=True))
        for c in range(length):
            for kind in range(2):
                value = got_ref[c, kind * exp_dev:(kind + 1) * exp_dev, :]
                for i in range(1, far + 1):
                    line = (2 * (i - 1) + kind) * exp_dev
                    column = place + jnp.where(place < reach, reach + i, -reach - i)
                    value += jnp.where(c == column, guest_ref[0, line:line + exp_dev, :], 0.0)
                if kind:
                    value += jnp.where(c == place, late_ref[...], 0.0)
                at = 2 * c + jnp.where(side == kind, 0, 1)
                dots_ref[pl.ds(at, 1), :, :] = value[None]
        dots = jnp.concatenate([dots_ref[j] for j in range(ep)], axis=0)
        mixed = mix_ref[...] * dots
        grad = (spread + (mixed - mix_ref[...] * jnp.sum(mixed, axis=0, keepdims=True))).astype(BF16)
        grad_ref[...] = grad
        term = jnp.dot(grad, tokens_ref[...], preferred_element_type=F32)
        for d in range(dp):
            part = term[:, d * piece:(d + 1) * piece]
            for j in range(ep):
                sent_ref[j * dp + d, :, :piece] = part[j * exp_dev:(j + 1) * exp_dev]
        sums = jnp.broadcast_to(sums_ref[...][None], (ep * dp, exp_dev, experts))
        sent_ref[:, :, piece:piece + experts] = sums
        if lanes > piece + experts:
            sent_ref[:, :, piece + experts:] = jnp.zeros((ep * dp, exp_dev, lanes - piece - experts), F32)

    return pl.pallas_call(
        body,
        in_specs=[SCALARS] + [LOCAL] * 8,
        out_specs=[LOCAL] * 2,
        out_shape=[
            jax.ShapeDtypeStruct((experts, tok), BF16),
            jax.ShapeDtypeStruct((ep * dp, exp_dev, lanes), F32),
        ],
        scratch_shapes=[pltpu.VMEM((ep, exp_dev, tok), F32)],
        cost_estimate=pl.CostEstimate(
            flops=2 * experts * tok * width, bytes_accessed=2 * tok * width + 4 * experts * width, transcendentals=0
        ),
        name="finish",
    )(scale, got, guest, late, mix, probability, counts, prob_sums, tokens)


def on_device(tokens, out_grad, indices, expert_rows, router_weight, router_bias, balance_scale):
    tok, width = tokens.shape
    experts = router_weight.shape[1]
    exp_dev, capacity = expert_rows.shape[1], expert_rows.shape[3]
    ep, dp = lax.axis_size("ep"), lax.axis_size("dp")
    token_total = tok * ep * dp
    assert ep % 4 == 0
    length = ep // 2
    reach = length // 2
    far = length - 1 - reach

    entries = exp_dev * capacity
    table = expert_rows.transpose(0, 1, 3, 2, 4).reshape(entries * ep, width)
    cross = [(j, j ^ 1) for j in range(ep)]
    leaving = list(split_rows(table, [(0, True)], ep))
    table, leaving[0] = lax.optimization_barrier((table, leaving[0]))
    block = out_grad
    rest = list(split_rows(table, [(n, True) for n in range(1, length)] + [(n, False) for n in range(length)], ep))
    leaving, own = leaving + rest[:length - 1], rest[length - 1:]

    chosen, _ = lax.optimization_barrier((indices.T, rest[0]))
    mine = slot_marks(chosen, ep, exp_dev)
    marks = lax.all_to_all(mine, "ep", split_axis=0, concat_axis=0, tiled=True)
    counts = jnp.sum((marks >= 0).astype(F32), axis=(0, 3)).reshape(1, experts)
    counts = lax.all_to_all(jnp.broadcast_to(counts, (dp, experts)), "dp", split_axis=0, concat_axis=0, tiled=True)

    size = min(entries, -(-capacity * (exp_dev - 1) // 16) * 16)
    leaving[-2:] = pack_rows(leaving[-2:], [length - 2, length - 1], marks, exp_dev, size)
    other = []
    for rows in leaving:
        other.append(lax.ppermute(rows, "ep", cross))

    def shift(x, *moves):
        pairs = [(z, to) for valid, by in moves for z in range(length) for to in [z + by] if valid(z) and 0 <= to < length]
        return lax.ppermute(x, "ep", [(2 * z + s, 2 * to + s) for z, to in pairs for s in range(2)])

    below, above = [block], [block]
    for hop in range(reach):
        below.append(shift(below[-1], (lambda z: z >= hop, 1)))
        above.append(shift(above[-1], (lambda z: z + hop < length, -1)))
    blocks = below[:0:-1] + [block] + above[1:]

    guests = []
    for i in range(1, far + 1):
        d = reach + i
        moves = ((lambda z: z + d < length, i), (lambda z: z - d >= 0, -i))
        guests.append([])
        for rows in (own, other):
            guests[-1].append(shift(rows[length - 1 - d], *moves))

    tokens, _ = lax.optimization_barrier((tokens, rest[0]))
    probability, mix, prob_sums = router(router_weight.T, tokens, router_bias[:, None], mine[0])

    def job(n, kinds, hops):
        def plan():
            _, place, _ = spot(length)
            source = source_at(length, n)
            return source, place, source - place + hops, source

        return [(own, other)[kind][n] for kind in kinds], kinds, plan, 0, 0

    def guest_job(i, kind):
        def plan():
            _, place, low = spot(length)
            column = place + jnp.where(low, -i, i)
            source = place + jnp.where(low, reach, -reach)
            there = (column >= 0) & (column < length)
            which = jnp.where(there, jnp.where(low, 2 * reach, 0), -1)
            return source, jnp.clip(column, 0, length - 1), which, 0

        return [guests[i - 1][kind]], (kind,), plan, 2 * (i - 1) * exp_dev, 1

    message = jnp.zeros((length, 2 * exp_dev, tok), F32)
    guest = jnp.zeros((1, 2 * exp_dev * far, tok), F32)
    near = [job(0, (0, 1), 1), job(length - 2, (0,), 1), job(length - 1, (0,), 1)]
    message, = meet(blocks[reach - 1:reach + 2], near, marks, [message], exp_dev, entries)
    with_guests = [job(n, (0, 1), reach) for n in range(1, length - 2)] + [guest_job(i, 0) for i in range(1, far + 1)]
    message, guest = meet(blocks, with_guests, marks, [message, guest], exp_dev, entries)
    late_jobs = [job(length - 2, (1,), reach)] + [guest_job(i, 1) for i in range(1, far + 1)]
    message, guest = meet(blocks, late_jobs, marks, [message, guest], exp_dev, entries)
    rows_of = [[2 * z + s for z in range(length)] for s in range(2)]
    got = lax.all_to_all(message, "ep", split_axis=0, concat_axis=0, tiled=True, axis_index_groups=rows_of)
    guest = shift(guest, (lambda z: 0 < z < reach, reach), (lambda z: reach <= z < length - 1, -reach))
    late = last_dots(out_grad, other[length - 1], marks, exp_dev, entries)

    share = 1.0 / (token_total * indices.shape[1])
    logit_grad, sent = finish(
        got, guest, late, mix, probability, counts, balance_scale, prob_sums, tokens, dp, exp_dev, share
    )
    token_grad = lax.dot_general(
        logit_grad, router_weight, (((0,), (1,)), ((), ())), preferred_element_type=F32
    ).astype(BF16)
    summed = jnp.sum(lax.all_to_all(sent, ("ep", "dp"), split_axis=0, concat_axis=0, tiled=True), axis=0)
    share_of = jnp.sum(counts, axis=0) * share
    piece = width // dp
    weight_grad = summed[:, :piece].T / math.sqrt(token_total)
    balance_loss = (experts * jnp.sum(share_of * (summed[0, piece:piece + experts] / token_total))).reshape(1)
    return (token_grad, weight_grad, balance_loss)


def solution(mesh):
    placed = (
        P(("ep", "dp"), None),
        P(("ep", "dp"), None),
        P(("ep", "dp"), None),
        P("dp", "ep", None, None, None),
        P(),
        P(),
        P(),
    )

    return jax.shard_map(
        on_device,
        mesh=mesh,
        in_specs=placed,
        out_specs=(P(("ep", "dp"), None), P("dp", "ep"), P()),
        check_vma=False,
    )
```
